32 devices in a mesh: table: 8 (over y, x, core), batch: 4 (over z).
Axes of the slice: x: 2, y: 2, z: 4, core: 2. Of those that a mesh axis runs over, the one named last changes fastest.
Arguments:
- queries: bfloat16 [128, 4, 512], P(('table', 'batch')), may hold values from -5 to 5
- indices: int32 [128, 4, 32], P(('table', 'batch')), may hold values from 0 to 262143, as said below
- first_keys: bfloat16 [4, 256, 256], P(None, ('table', 'batch')), may hold values from -4 to 4
- second_keys: bfloat16 [4, 1024, 256], replicated, may hold values from -4 to 4
- values: bfloat16 [262144, 1024], P(('table', 'batch')), may hold values from -6 to 6
Outputs:
- memory_read: bfloat16 [128, 1024], P(('table', 'batch'))
The draws below stay inside these ranges and needn't reach their ends.
Inputs may be any that keep to these rules, and one draw needn't show every extreme that they name: `indices`: row r of the value table belongs to device r // 8192 of table+batch. The entries of the 4 sequences of one device name rows of any one owner at most 32 times, and one owner is named exactly 32 times by the entries of every device.
All inputs are finite; a program needn't handle non-finite values.
Results may differ from the reference program's by a relative error of at most 0.005.
Values may be sent and summed in bfloat16 or wider, within the bound.
A program may use at most 64 MiB of HBM per device.

```python
import math
import jax
import jax.numpy as jnp

HEADS = 4
KDIM = 512
HALF = 256
NSUB = 1024
DV = 1024
VALS_DEV = 8192
TOPK = 32
ROWS = 262144
NFIRST = 256
SEQS = 128
ENTRIES = 512
CAP = 32
DEVICES = 32


def owner_table(key):
    base_key = jax.random.fold_in(key, 101)
    hot_owner = jax.random.randint(jax.random.fold_in(base_key, 1), (), 0, DEVICES).astype(jnp.int32)
    others = (hot_owner + 1 + jnp.arange(DEVICES - 1, dtype=jnp.int32)) % DEVICES
    deck_cards = jnp.repeat(others, CAP)
    block_keys = jax.random.split(jax.random.fold_in(base_key, 2), DEVICES)

    def one_block(block_key):
        deal_key, mix_key, row_key = jax.random.split(block_key, 3)
        dealt = jax.random.permutation(deal_key, deck_cards)[:ENTRIES - CAP]
        owners = jnp.concatenate([jnp.zeros((CAP,), jnp.int32) + hot_owner, dealt.astype(jnp.int32)])
        owners = jax.random.permutation(mix_key, owners)
        picked = jax.random.randint(row_key, (ENTRIES,), 0, VALS_DEV).astype(jnp.int32)
        return owners * VALS_DEV + picked
    blocks = jax.vmap(one_block)(block_keys)
    return blocks.reshape(SEQS, HEADS, TOPK).astype(jnp.int32)


def key_table(key, marker, count):
    sub_key = jax.random.fold_in(key, marker)
    drawn = jnp.clip(jax.random.normal(sub_key, (HEADS, count, HALF), jnp.float32), -4.0, 4.0)
    return drawn.astype(jnp.bfloat16)


def draw_indices(key, part):
    return owner_table(key)


def draw_first_keys(key, part):
    return key_table(key, 202, NFIRST)


def draw_second_keys(key, part):
    return key_table(key, 303, NSUB)


def draw_queries(key, part):
    drawn_key = jax.random.fold_in(key, 404)
    spread = 1.4 / math.sqrt(KDIM)
    entries = jnp.clip(jax.random.normal(drawn_key, (SEQS, HEADS, KDIM), jnp.float32), -6.0, 6.0) * spread
    return entries.astype(jnp.bfloat16)


def level_of(stream_key, extent, shards, low, top_value):
    level = 1.0
    for position, blocks in shards:
        draws = jax.random.uniform(jax.random.fold_in(jax.random.fold_in(stream_key, 6), position), (blocks,), jnp.float32, low / len(shards), top_value / len(shards))
        level = level * jnp.repeat(jnp.exp(draws), extent[position] // blocks).reshape((-1,) + (1,) * (len(extent) - 1 - position))
    return level


def noise(own_key, extent, deviation, bound, cuts=(), held_as=jnp.bfloat16):
    values = deviation * jax.random.normal(own_key, extent, jnp.float32)
    if cuts:
        values = values * level_of(own_key, extent, cuts, -0.22, 0.18)
    return jnp.clip(values, -bound, bound).astype(held_as)


def setup_inputs(seed: int = 0) -> dict:
    key_list = jax.random.split(jax.random.key(seed), 6)
    return {
        "queries": draw_queries(jax.random.fold_in(key_list[5], 71), 0),
        "indices": draw_indices(jax.random.fold_in(key_list[5], 71), 0),
        "first_keys": draw_first_keys(jax.random.fold_in(key_list[5], 71), 0),
        "second_keys": draw_second_keys(jax.random.fold_in(key_list[5], 71), 0),
        "values": noise(key_list[4], (ROWS, DV), 1.0, 6.0, ((0, 32),)),
    }


def reference(queries, indices, first_keys, second_keys, values):
    head_ids = jnp.arange(HEADS, dtype=jnp.int32)[None, :, None]
    first_ids = (indices // NSUB).astype(jnp.int32)
    second_ids = (indices % NSUB).astype(jnp.int32)
    query_first = queries[:, :, :HALF].astype(jnp.float32)
    query_second = queries[:, :, HALF:].astype(jnp.float32)
    first_rows = first_keys[head_ids, first_ids].astype(jnp.float32)
    second_rows = second_keys[head_ids, second_ids].astype(jnp.float32)
    first_part = jnp.sum(query_first[:, :, None, :] * first_rows, axis=-1)
    second_part = jnp.sum(query_second[:, :, None, :] * second_rows, axis=-1)
    weights = jax.nn.softmax(first_part + second_part, axis=-1).astype(jnp.bfloat16)
    result = jnp.zeros((SEQS, DV), jnp.float32)
    for head_index in range(HEADS):
        fetched = values[indices[:, head_index]].astype(jnp.float32)
        result = result + jnp.einsum("sk,skd->sd", weights[:, head_index].astype(jnp.float32), fetched)
    return result.astype(jnp.bfloat16)
```

```python
import functools

import jax
import jax.numpy as jnp
from jax import lax
from jax.experimental import pallas as pl
from jax.experimental.pallas import tpu as pltpu
from jax.sharding import PartitionSpec as P

MESH = pl.DeviceIdType.MESH
LANES = 128
NT = (((1,), (1,)), ((), ()))
NN = (((1,), (0,)), ((), ()))


def log2(number):
    assert number & (number - 1) == 0
    return number.bit_length() - 1


def pick_lanes(table, ids):
    picked = jnp.zeros(ids.shape, jnp.float32)
    inner = ids & (LANES - 1)
    outer = lax.shift_right_arithmetic(ids, 7)
    for part in range(table.shape[1] // LANES):
        got = jnp.take_along_axis(table[:, part * LANES : (part + 1) * LANES], inner, axis=1)
        picked = jnp.where(outer == part, got, picked)
    return picked


def kernel(
    shape,
    q_hbm,
    i_hbm,
    fk_hbm,
    sk_ref,
    v_ref,
    out_ref,
    q_ref,
    i_ref,
    fk_ref,
    vbuf,
    k2buf,
    kslot,
    islot,
    gslot,
    icomp,
    qslot,
    qrows,
    grows,
    rolled,
    wpack,
    wslot,
    istage,
    wstage,
    wfin,
    wacc,
    wb,
    lows,
    accs,
    pair,
    psend,
    pslot,
    in_sem,
    v_sem,
    k2_sem,
    k_send,
    k_recv,
    i_send,
    i_recv,
    r_send,
    r_recv,
    g_send,
    g_recv,
    q_send,
    q_recv,
    w_send,
    w_recv,
    a_send,
    a_recv,
    p_send,
    p_recv,
):
    nt, nb, heads, seqs, top, chunks, pieces, early = shape
    devices = nt * nb
    groups = devices // heads
    half = q_ref.shape[2] // 2
    rows, width = v_ref.shape
    t_me, b_me = lax.axis_index("table"), lax.axis_index("batch")
    dev_me = t_me * nb + b_me
    core_me = lax.rem(t_me, 2)
    head_me = lax.rem(t_me, heads)
    group_me = lax.div(t_me, heads) * nb + b_me
    slot_me = head_me * groups + group_me

    def flips(x, count):
        bits = [(x // 2**i) % 2 for i in range(log2(count))]
        return [
            x + sum((1 - 2 * bit) * 2**i for i, bit in enumerate(bits) if mask >> i & 1)
            for mask in range(count)
        ]

    t_flips, b_flips = flips(t_me, nt), flips(b_me, nb)
    t_heads = [lax.rem(t, heads) for t in t_flips]
    t_slots = [h * groups + lax.div(t, heads) * nb for t, h in zip(t_flips, t_heads)]
    masks = sorted(
        ((mt, mb) for mt in range(nt) for mb in range(nb) if mt or mb),
        key=lambda m: (m[1] + bin(m[0] >> 1).count("1"), m),
        reverse=True,
    )

    def others(body, stride=1):
        for mt, mb in masks:
            if mt % stride == 0:
                body(t_slots[mt] + b_flips[mb], (t_flips[mt], b_flips[mb]), t_heads[mt])

    def drain(ref, sem):
        pltpu.make_async_copy(ref, ref, sem).wait()

    barrier = pltpu.get_barrier_semaphore()
    others(
        lambda slot, where, head: pl.semaphore_signal(
            barrier, inc=1, device_id=where, device_id_type=MESH
        )
    )
    in_copies = [
        pltpu.make_async_copy(src, dst, in_sem.at[n])
        for n, (src, dst) in enumerate(((i_hbm, i_ref), (fk_hbm, fk_ref), (q_hbm, q_ref)))
    ]
    for copy in in_copies:
        copy.start()
    k2_copy = pltpu.make_async_copy(sk_ref.at[head_me], k2buf, k2_sem)
    k2_copy.start()
    block = rows // pieces
    v_copies = [
        pltpu.make_async_copy(
            v_ref.at[pl.ds(p * block, block)], vbuf.at[pl.ds(p * block, block)], v_sem.at[p]
        )
        for p in range(pieces)
    ]
    for copy in v_copies:
        copy.start()

    for copy in in_copies:
        copy.wait()
    for h in range(heads):
        for s in range(seqs):
            icomp[pl.ds(s, 1), pl.ds(h * top, top)] = i_ref[s, pl.ds(h, 1), :]
    islot[slot_me] = icomp[...]
    kslot[dev_me] = fk_ref[head_me]
    gslot[head_me] = icomp[...]
    qslot[head_me] = q_ref[...]
    pl.semaphore_wait(barrier, devices - 1)

    def send_q(j):
        other = lax.rem(head_me + j, heads)
        pltpu.make_async_remote_copy(
            src_ref=q_ref,
            dst_ref=qslot.at[head_me],
            send_sem=q_send,
            recv_sem=q_recv,
            device_id=(lax.div(t_me, heads) * heads + other, b_me),
            device_id_type=MESH,
        ).start()

    def send_group_ids(j):
        other = lax.rem(head_me + j, heads)
        pltpu.make_async_remote_copy(
            src_ref=icomp,
            dst_ref=gslot.at[head_me],
            send_sem=g_send,
            recv_sem=g_recv,
            device_id=(lax.div(t_me, heads) * heads + other, b_me),
            device_id_type=MESH,
        ).start()

    for j in range(1, heads):
        send_q(j)
        send_group_ids(j)

    def send_keys(slot, where, head):
        pltpu.make_async_remote_copy(
            src_ref=fk_ref.at[head],
            dst_ref=kslot.at[dev_me],
            send_sem=k_send,
            recv_sem=k_recv,
            device_id=where,
            device_id_type=MESH,
        ).start()

    def send_ids(slot, where, head):
        pltpu.make_async_remote_copy(
            src_ref=icomp,
            dst_ref=islot.at[slot_me],
            send_sem=i_send,
            recv_sem=i_recv,
            device_id=where,
            device_id_type=MESH,
        ).start()

    others(send_keys)
    others(send_ids)

    drain(qslot.at[pl.ds(0, heads - 1)], q_recv)
    for j in range(heads):
        for s in range(seqs):
            one = qslot[j, s].astype(jnp.float32)
            for c in range(qrows.shape[0]):
                qrows[c, pl.ds((j * seqs + s) * heads, heads), :] = one[
                    :, c * LANES : (c + 1) * LANES
                ]
    q_all = jnp.concatenate(
        [
            qrows.at[c][pl.ds(head_me, heads * seqs, stride=heads), :]
            for c in range(qrows.shape[0])
        ],
        axis=1,
    ).astype(jnp.bfloat16)
    k2_copy.wait()
    s2 = lax.dot_general(q_all[:, half:], k2buf[...], NT, preferred_element_type=jnp.float32)
    drain(gslot.at[pl.ds(0, heads - 1)], g_recv)
    for j in range(heads):
        grows[pl.ds(j * seqs, seqs), :] = gslot[j]
    ids = grows[...]
    sub_count = k2buf.shape[0]
    second = pick_lanes(s2, ids & (sub_count - 1))
    drain(kslot.at[pl.ds(0, devices - 1)], k_recv)
    k1 = kslot[...].astype(jnp.float32)
    k1 = k1.reshape(k1.shape[0] * k1.shape[1], half).astype(jnp.bfloat16)
    s1 = lax.dot_general(q_all[:, :half], k1, NT, preferred_element_type=jnp.float32)
    score = second + pick_lanes(s1, lax.shift_right_arithmetic(ids, log2(sub_count)))
    lane = lax.broadcasted_iota(jnp.int32, ids.shape, 1)
    mine = lax.shift_right_arithmetic(lane, log2(top)) == head_me
    best = jnp.max(jnp.where(mine, score, -jnp.inf), axis=1, keepdims=True)
    raised = jnp.where(mine, jnp.exp(jnp.where(mine, score - best, 0.0)), 0.0)
    weights = raised / jnp.sum(raised, axis=1, keepdims=True)
    weights = weights.astype(jnp.bfloat16).astype(jnp.float32)
    for j in range(heads):
        rolled[j] = pltpu.roll(weights, lax.rem(j - head_me + heads, heads) * top, 1)
    packed = rolled[0, pl.ds(0, seqs), :]
    for j in range(1, heads):
        packed = packed + rolled[j, pl.ds(j * seqs, seqs), :]
    wpack[...] = packed
    wslot[slot_me] = packed

    def send_weights(slot, where, head):
        pltpu.make_async_remote_copy(
            src_ref=wpack,
            dst_ref=wslot.at[slot_me],
            send_sem=w_send,
            recv_sem=w_recv,
            device_id=where,
            device_id_type=MESH,
        ).start()

    others(send_weights)
    high_count = rows // LANES
    all_seqs = devices * seqs
    high_iota = lax.broadcasted_iota(jnp.int32, (high_count, LANES), 0)
    low_iota = lax.broadcasted_iota(jnp.int32, (LANES, LANES), 0)
    base = dev_me * rows

    def high_hot(s, value):
        high = lax.shift_right_arithmetic(istage[pl.ds(s, 1), :] - base, 7)
        return jnp.where(high_iota == high, value, 0.0).astype(jnp.bfloat16)

    def low_hot(s):
        low = istage[pl.ds(s, 1), :] & (LANES - 1)
        return jnp.where(low_iota == low, 1.0, 0.0).astype(jnp.bfloat16)

    drain(islot.at[pl.ds(0, devices - 1)], i_recv)
    for slot in range(devices):
        istage[pl.ds(slot * seqs, seqs), :] = islot[slot]
    low_lane = lax.broadcasted_iota(jnp.int32, (LANES, LANES), 1).astype(jnp.float32)
    if early:

        def build(step, carry):
            some = istage[pl.ds(pl.multiple_of(step * 8, 8), 8), :] & (LANES - 1)
            some = some.astype(jnp.float32).T
            for u in range(8):
                hot = jnp.where(low_lane == some[:, u : u + 1], 1.0, 0.0)
                lows[step * 8 + u] = hot.astype(jnp.bfloat16)
            return carry

        lax.fori_loop(0, all_seqs // 8, build, 0)
    drain(wslot.at[pl.ds(0, devices - 1)], w_recv)
    for slot in range(devices):
        wstage[pl.ds(slot * seqs, seqs), :] = wslot[slot]
    span = groups * seqs
    lane = lax.broadcasted_iota(jnp.int32, (span, LANES), 1)
    block_of = lax.shift_right_arithmetic(lane, log2(top))
    for j in range(heads):
        total = jnp.zeros((span, LANES), jnp.float32)
        for h in range(heads):
            part = wstage[pl.ds(h * span, span), :]
            if h != j:
                part = pltpu.roll(part, (h - j) % heads * top, 1)
            total = jnp.where(block_of == h, part, total)
        wfin[pl.ds(j * span, span), :] = total

    pitch = all_seqs + 8

    def spread(step, carry):
        for u in range(32):
            s = step * 32 + u
            left = high_hot(s, wfin[pl.ds(s, 1), :])
            right = lows[s] if early else low_hot(s)
            wacc[pl.ds(s, high_count, stride=pitch), :] = lax.dot_general(
                left, right, NN if early else NT, preferred_element_type=jnp.float32
            )
        return carry

    lax.fori_loop(0, all_seqs // 32, spread, 0)

    def narrow(step, carry):
        wb[:, pl.ds(pl.multiple_of(step * LANES, LANES), LANES)] = wacc[
            pl.ds(pl.multiple_of(step * pitch, 8), all_seqs), :
        ].astype(jnp.bfloat16)
        return carry

    lax.fori_loop(0, high_count, narrow, 0, unroll=8)
    for copy in v_copies:
        copy.wait()

    piece = width // chunks
    half_slot = lax.div(head_me, 2) * groups + group_me

    def pass_on(c):
        drain(pair.at[c], a_recv.at[c])
        for i in range(heads // 2):
            both = accs[c, 2 * i + core_me] + pair[c, i]
            for g in range(groups):
                psend[c, i * groups + g] = both[g * seqs : (g + 1) * seqs, :].astype(jnp.bfloat16)
        pslot[c, half_slot] = psend[c, half_slot]

        def send_part(slot, where, head):
            pltpu.make_async_remote_copy(
                src_ref=psend.at[c, slot - lax.div(head + 1, 2) * groups],
                dst_ref=pslot.at[c, half_slot],
                send_sem=p_send.at[c],
                recv_sem=p_recv.at[c],
                device_id=where,
                device_id_type=MESH,
            ).start()

        others(send_part, 2)

    for c in range(chunks):
        acc = jnp.dot(
            wb[...], vbuf[:, pl.ds(c * piece, piece)], preferred_element_type=jnp.float32
        )
        for j in range(heads):
            accs[c, j] = acc[j * span : (j + 1) * span, :]
        for i in range(heads // 2):
            pltpu.make_async_remote_copy(
                src_ref=accs.at[c, 2 * i + 1 - core_me],
                dst_ref=pair.at[c, i],
                send_sem=a_send.at[c],
                recv_sem=a_recv.at[c],
                device_id=(t_me + 1 - 2 * core_me, b_me),
                device_id_type=MESH,
            ).start()
        if c > 0:
            pass_on(c - 1)
    pass_on(chunks - 1)

    for c in range(chunks):
        drain(pslot.at[c, pl.ds(0, devices // 2 - 1)], p_recv.at[c])
        total = jnp.zeros((seqs, piece), jnp.float32)
        for slot in range(devices // 2):
            total = total + pslot[c, slot].astype(jnp.float32)
        out_ref[:, pl.ds(c * piece, piece)] = total.astype(jnp.bfloat16)

    drain(qslot.at[pl.ds(0, heads - 1)], q_send)
    drain(gslot.at[pl.ds(0, heads - 1)], g_send)
    drain(kslot.at[pl.ds(0, devices - 1)], k_send)
    drain(islot.at[pl.ds(0, devices - 1)], i_send)
    drain(wslot.at[pl.ds(0, devices - 1)], w_send)
    for c in range(chunks):
        drain(pslot.at[c, pl.ds(0, devices // 2 - 1)], p_send.at[c])
        drain(pair.at[c], a_send.at[c])


def shards(nt, nb, queries, indices, first_keys, second_keys, values):
    seqs, heads, top = indices.shape
    width_q = queries.shape[2]
    half = width_q // 2
    firsts = first_keys.shape[1]
    sub_count = second_keys.shape[1]
    rows, width = values.shape
    devices = nt * nb
    all_seqs = devices * seqs
    assert heads * top == LANES and nt % heads == 0 and heads % 2 == 0
    chunks, pieces = 2, 4
    early = all_seqs <= 256
    vmem = pl.BlockSpec(memory_space=pltpu.VMEM)
    hbm = pl.BlockSpec(memory_space=pltpu.MemorySpace.HBM)
    dma = pltpu.SemaphoreType.DMA
    return pl.pallas_call(
        functools.partial(kernel, (nt, nb, heads, seqs, top, chunks, pieces, early)),
        out_shape=pltpu.VMEM((seqs, width), jnp.bfloat16),
        in_specs=[hbm] * 5,
        out_specs=vmem,
        scratch_shapes=[
            pltpu.VMEM(queries.shape, queries.dtype),
            pltpu.VMEM(indices.shape, indices.dtype),
            pltpu.VMEM(first_keys.shape, first_keys.dtype),
            pltpu.VMEM((rows, width), jnp.bfloat16),
            pltpu.VMEM((sub_count, half), jnp.bfloat16),
            pltpu.VMEM((devices, firsts, half), jnp.bfloat16),
            pltpu.VMEM((devices, seqs, LANES), jnp.int32),
            pltpu.VMEM((heads, seqs, LANES), jnp.int32),
            pltpu.VMEM((seqs, LANES), jnp.int32),
            pltpu.VMEM((heads, seqs, heads, width_q), jnp.bfloat16),
            pltpu.VMEM((width_q // LANES, heads * seqs * heads, LANES), jnp.float32),
            pltpu.VMEM((heads * seqs, LANES), jnp.int32),
            pltpu.VMEM((heads, heads * seqs, LANES), jnp.float32),
            pltpu.VMEM((seqs, LANES), jnp.float32),
            pltpu.VMEM((devices, seqs, LANES), jnp.float32),
            pltpu.VMEM((all_seqs, LANES), jnp.int32),
            pltpu.VMEM((all_seqs, LANES), jnp.float32),
            pltpu.VMEM((all_seqs, LANES), jnp.float32),
            pltpu.VMEM((rows // LANES * (all_seqs + 8), LANES), jnp.float32),
            pltpu.VMEM((all_seqs, rows), jnp.bfloat16),
            pltpu.VMEM((all_seqs if early else 1, LANES, LANES), jnp.bfloat16),
            pltpu.VMEM((chunks, heads, all_seqs // heads, width // chunks), jnp.float32),
            pltpu.VMEM((chunks, heads // 2, all_seqs // heads, width // chunks), jnp.float32),
            pltpu.VMEM((chunks, devices // 2, seqs, width // chunks), jnp.bfloat16),
            pltpu.VMEM((chunks, devices // 2, seqs, width // chunks), jnp.bfloat16),
            dma((3,)),
            dma((pieces,)),
            dma,
            dma,
            dma,
            dma,
            dma,
            dma,
            dma,
            dma,
            dma,
            dma,
            dma,
            dma,
            dma,
            dma((chunks,)),
            dma((chunks,)),
            dma((chunks,)),
            dma((chunks,)),
        ],
        compiler_params=pltpu.CompilerParams(
            collective_id=0, has_side_effects=True, vmem_limit_bytes=56 * 1024 * 1024
        ),
    )(queries, indices, first_keys, second_keys, values)


def solution(mesh):
    placed = (
        P(("table", "batch"), None, None),
        P(("table", "batch"), None, None),
        P(None, ("table", "batch"), None),
        P(),
        P(("table", "batch"), None),
    )
    body = functools.partial(shards, mesh.shape["table"], mesh.shape["batch"])
    return jax.shard_map(
        body, mesh=mesh, in_specs=placed, out_specs=P(("table", "batch"), None), check_vma=False
    )
```

```python
import functools

import jax
import jax.numpy as jnp
from jax import lax
from jax.experimental import pallas as pl
from jax.experimental.pallas import tpu as pltpu
from jax.sharding import PartitionSpec as P

MESH = pl.DeviceIdType.MESH
LANES = 128
NT = (((1,), (1,)), ((), ()))
NN = (((1,), (0,)), ((), ()))
WAVES = 2


def log2(number):
    assert number & (number - 1) == 0
    return number.bit_length() - 1


def pick_lanes(table, ids):
    picked = jnp.zeros(ids.shape, jnp.float32)
    inner = ids & (LANES - 1)
    outer = lax.shift_right_arithmetic(ids, 7)
    for part in range(table.shape[1] // LANES):
        got = jnp.take_along_axis(table[:, part * LANES : (part + 1) * LANES], inner, axis=1)
        picked = jnp.where(outer == part, got, picked)
    return picked


def kernel(
    shape,
    q_hbm,
    i_hbm,
    fk_hbm,
    sk_hbm,
    v_hbm,
    out_ref,
    q_ref,
    i_ref,
    fk_ref,
    vbuf,
    k2buf,
    kslot,
    islot,
    icomp,
    qrows,
    qsend,
    qslot,
    qstage,
    wpack,
    wslot,
    istage,
    wfin,
    wacc,
    wb,
    highs,
    lows,
    accs,
    pair,
    psend,
    pslot,
    ready,
    in_sem,
    v_sem,
    k2_sem,
    k_send,
    k_recv,
    i_send,
    i_recv,
    q_send,
    q_recv,
    w_send,
    w_recv,
    a_send,
    a_recv,
    p_send,
    p_recv,
):
    nt, nb, heads, seqs, top, chunks, pieces, early = shape
    devices = nt * nb
    quads = nt // heads
    deep = nb // WAVES
    middles = (deep - 1, deep)
    span = deep * seqs
    block_rows = quads * span
    wave_rows = heads * block_rows
    wave_devs = nt * deep
    all_seqs = devices * seqs
    half = fk_hbm.shape[2]
    rows, width = v_hbm.shape
    high_count = rows // LANES
    pitch = all_seqs + 8
    t_me, b_me = lax.axis_index("table"), lax.axis_index("batch")
    dev_me = t_me * nb + b_me
    core_me = lax.rem(t_me, 2)
    head_me = lax.rem(t_me, heads)
    quad_me = lax.div(t_me, heads)
    wave_me = lax.div(b_me, deep)
    deep_me = lax.rem(b_me, deep)
    middle_me = deep - 1 + wave_me
    central = b_me == middle_me

    def slot_of(t, b):
        return (
            lax.div(b, deep) * wave_devs
            + (lax.rem(t, heads) * quads + lax.div(t, heads)) * deep
            + lax.rem(b, deep)
        )

    def flips(x, count):
        bits = [(x // 2**i) % 2 for i in range(log2(count))]
        return [
            x + sum((1 - 2 * bit) * 2**i for i, bit in enumerate(bits) if mask >> i & 1)
            for mask in range(count)
        ]

    slot_me = slot_of(t_me, b_me)
    t_flips = flips(t_me, nt)
    deep_flips = flips(deep_me, deep)
    t_masks = sorted(range(nt), key=lambda m: (bin(m >> 1).count("1"), m), reverse=True)

    def unless_me(mt, k, body):
        if mt:
            body()
        else:
            pl.when(b_me != k)(body)

    def drain(ref, sem):
        pltpu.make_async_copy(ref, ref, sem).wait()

    def drain_count(less, ref_of, count, sem):
        pl.when(less)(lambda: drain(ref_of(count - 1), sem))
        pl.when(jnp.logical_not(less))(lambda: drain(ref_of(count), sem))

    def remote(src, dst, send, recv, where):
        pltpu.make_async_remote_copy(
            src_ref=src,
            dst_ref=dst,
            send_sem=send,
            recv_sem=recv,
            device_id=where,
            device_id_type=MESH,
        ).start()

    barrier = pltpu.get_barrier_semaphore()

    def greet(sem, where):
        pl.semaphore_signal(sem, inc=1, device_id=where, device_id_type=MESH)

    for k in range(nb - 1, -1, -1):

        @pl.when(b_me <= k)
        def _():
            for mt in t_masks:
                unless_me(mt, k, lambda mt=mt: greet(barrier, (t_flips[mt], k)))

    in_copies = [
        pltpu.make_async_copy(src, dst, in_sem.at[n])
        for n, (src, dst) in enumerate(((i_hbm, i_ref), (fk_hbm, fk_ref), (q_hbm, q_ref)))
    ]
    for copy in in_copies:
        copy.start()
    pl.semaphore_wait(barrier, nt * (b_me + 1) - 1)
    for k in range(nb - 1):

        @pl.when(b_me > k)
        def _():
            for mt in t_masks:
                greet(ready.at[b_me], (t_flips[mt], k))

    for copy in in_copies:
        copy.wait()
    k2_copy = pltpu.make_async_copy(sk_hbm.at[head_me], k2buf, k2_sem)
    k2_copy.start()
    block = rows // pieces
    v_copies = [
        pltpu.make_async_copy(
            v_hbm.at[pl.ds(p * block, block)], vbuf.at[pl.ds(p * block, block)], v_sem.at[p]
        )
        for p in range(pieces)
    ]
    for copy in v_copies:
        copy.start()

    for h in range(heads):
        for s in range(seqs):
            icomp[pl.ds(s, 1), pl.ds(h * top, top)] = i_ref[s, pl.ds(h, 1), :]
    islot[slot_me] = icomp[...]
    kslot[dev_me] = fk_ref[head_me]
    for s in range(seqs):
        one = q_ref[s].astype(jnp.float32)
        for h in range(heads):
            qrows[h, pl.ds(s, 1), :] = one[h : h + 1, :]
    for h in range(heads):
        qsend[h] = qrows[h].astype(jnp.bfloat16)
    place_me = head_me * deep + deep_me
    qslot[place_me] = qsend[head_me]

    for k in (*middles, *(k for k in range(nb) if k not in middles)):

        @pl.when(b_me < k)
        def _():
            pl.semaphore_wait(ready.at[k], nt)

        if k in middles:

            @pl.when(middle_me == k)
            def _():
                for h in range(heads):

                    @pl.when(jnp.logical_not(jnp.logical_and(central, head_me == h)))
                    def _():
                        remote(
                            qsend.at[h],
                            qslot.at[place_me],
                            q_send,
                            q_recv,
                            (quad_me * heads + h, k),
                        )

            for mt in t_masks:
                unless_me(
                    mt,
                    k,
                    lambda mt=mt, k=k: remote(
                        fk_ref.at[lax.rem(t_flips[mt], heads)],
                        kslot.at[dev_me],
                        k_send,
                        k_recv,
                        (t_flips[mt], k),
                    ),
                )
        for mt in t_masks:
            unless_me(
                mt,
                k,
                lambda mt=mt, k=k: remote(
                    icomp, islot.at[slot_me], i_send, i_recv.at[wave_me], (t_flips[mt], k)
                ),
            )

    def stage_ids(wave, mine):
        count = wave_devs - 1 if mine else wave_devs
        drain(islot.at[pl.ds(0, count)], i_recv.at[wave])
        for n in range(wave_devs):
            slot = wave * wave_devs + n
            istage[pl.ds(slot * seqs, seqs), :] = islot[slot]

    stage_ids(wave_me, True)
    k2_copy.wait()

    @pl.when(central)
    def _():
        places = heads * deep
        drain(qslot.at[pl.ds(0, places - 1)], q_recv)
        for n in range(places):
            qstage[pl.ds(n * seqs, seqs), :] = qslot[n].astype(jnp.float32)
        q_all = qstage[...].astype(jnp.bfloat16)
        s2 = lax.dot_general(q_all[:, half:], k2buf[...], NT, preferred_element_type=jnp.float32)
        ids = jnp.concatenate(
            [
                istage[
                    pl.ds(
                        pl.multiple_of(wave_me * wave_rows + j * block_rows + quad_me * span, 8),
                        span,
                    ),
                    :,
                ]
                for j in range(heads)
            ],
            axis=0,
        )
        sub_count = k2buf.shape[0]
        second = pick_lanes(s2, ids & (sub_count - 1))
        drain(kslot.at[pl.ds(0, devices - 1)], k_recv)
        k1 = kslot[...].astype(jnp.float32)
        k1 = k1.reshape(k1.shape[0] * k1.shape[1], half).astype(jnp.bfloat16)
        s1 = lax.dot_general(q_all[:, :half], k1, NT, preferred_element_type=jnp.float32)
        score = second + pick_lanes(s1, lax.shift_right_arithmetic(ids, log2(sub_count)))
        lane = lax.broadcasted_iota(jnp.int32, ids.shape, 1)
        mine = lax.shift_right_arithmetic(lane, log2(top)) == head_me
        best = jnp.max(jnp.where(mine, score, -jnp.inf), axis=1, keepdims=True)
        raised = jnp.where(mine, jnp.exp(jnp.where(mine, score - best, 0.0)), 0.0)
        weights = raised / jnp.sum(raised, axis=1, keepdims=True)
        weights = weights.astype(jnp.bfloat16).astype(jnp.float32)
        packed = jnp.zeros((span, LANES), jnp.float32)
        for j in range(heads):
            packed = packed + pltpu.roll(
                weights[j * span : (j + 1) * span, :],
                lax.rem(j - head_me + heads, heads) * top,
                1,
            )
        packed = packed.astype(jnp.bfloat16)
        wpack[...] = packed
        where_me = (wave_me * heads + head_me) * quads + quad_me
        wslot[where_me] = packed
        for k in sorted(range(nb), key=lambda k: abs(2 * k - nb + 1), reverse=True):
            for mt in t_masks:
                unless_me(
                    mt,
                    k,
                    lambda mt=mt, k=k: remote(
                        wpack, wslot.at[where_me], w_send, w_recv.at[wave_me], (t_flips[mt], k)
                    ),
                )

    high_iota = lax.broadcasted_iota(jnp.int32, (high_count, LANES), 0)
    low_iota = lax.broadcasted_iota(jnp.int32, (LANES, LANES), 0)
    low_lane = lax.broadcasted_iota(jnp.int32, (LANES, LANES), 1).astype(jnp.float32)
    base = dev_me * rows

    def high_hot(row):
        high = lax.shift_right_arithmetic(row - base, 7)
        return jnp.where(high_iota == high, 1.0, 0.0).astype(jnp.bfloat16)

    def build_masks(wave):
        def build(step, carry):
            first = pl.multiple_of(wave * wave_rows + step * 8, 8)
            some = istage[pl.ds(first, 8), :] & (LANES - 1)
            some = some.astype(jnp.float32).T
            for u in range(8):
                hot = jnp.where(low_lane == some[:, u : u + 1], 1.0, 0.0)
                lows[first + u] = hot.astype(jnp.bfloat16)
                highs[first + u] = high_hot(istage[pl.ds(first + u, 1), :])
            return carry

        lax.fori_loop(0, wave_rows // 8, build, 0)

    if early:
        build_masks(wave_me)
    stage_ids(1 - wave_me, False)
    if early:
        build_masks(1 - wave_me)

    piece = width // chunks
    chip_me = lax.div(t_me, 2) * nb + b_me
    chips = devices // 2
    lane = lax.broadcasted_iota(jnp.int32, (block_rows, LANES), 1)
    block_of = lax.shift_right_arithmetic(lane, log2(top))
    dest_masks = sorted(
        ((mt, mb) for mt in range(0, nt, 2) for mb in range(deep)),
        key=lambda m: (bin(m[0] >> 1).count("1") + m[1], m),
        reverse=True,
    )

    def weigh(w):
        n_w = heads * quads
        drain_count(
            jnp.logical_and(central, wave_me == w),
            lambda n: wslot.at[pl.ds(0, n)],
            n_w,
            w_recv.at[w],
        )
        parts = [
            wslot[pl.ds((w * heads + h) * quads, quads)]
            .astype(jnp.float32)
            .reshape(block_rows, LANES)
            for h in range(heads)
        ]
        for j in range(heads):
            total = jnp.zeros((block_rows, LANES), jnp.float32)
            for h in range(heads):
                part = parts[h]
                if h != j:
                    part = pltpu.roll(part, (h - j) % heads * top, 1)
                total = jnp.where(block_of == h, part, total)
            wfin[pl.ds(w * wave_rows + j * block_rows, block_rows), :] = total

        def spread(step, carry):
            for u in range(32):
                s = w * wave_rows + step * 32 + u
                weight = wfin[pl.ds(s, 1), :]
                if early:
                    left = highs[s] * jnp.broadcast_to(weight, (high_count, LANES)).astype(
                        jnp.bfloat16
                    )
                    got = lax.dot_general(left, lows[s], NN, preferred_element_type=jnp.float32)
                else:
                    row = istage[pl.ds(s, 1), :]
                    high = lax.shift_right_arithmetic(row - base, 7)
                    left = jnp.where(high_iota == high, weight, 0.0).astype(jnp.bfloat16)
                    low = jnp.where(low_iota == (row & (LANES - 1)), 1.0, 0.0)
                    got = lax.dot_general(
                        left, low.astype(jnp.bfloat16), NT, preferred_element_type=jnp.float32
                    )
                wacc[pl.ds(s, high_count, stride=pitch), :] = got
            return carry

        lax.fori_loop(0, wave_rows // 32, spread, 0)

        def narrow(step, carry):
            wb[
                pl.ds(w * wave_rows, wave_rows),
                pl.ds(pl.multiple_of(step * LANES, LANES), LANES),
            ] = wacc[
                pl.ds(pl.multiple_of(step * pitch + w * wave_rows, 8), wave_rows), :
            ].astype(jnp.bfloat16)
            return carry

        lax.fori_loop(0, high_count, narrow, 0, unroll=8)

    def multiply(c):
        acc = jnp.dot(
            wb[...], vbuf[:, pl.ds(c * piece, piece)], preferred_element_type=jnp.float32
        )
        for w in range(WAVES):
            for j in range(heads):
                first = w * wave_rows + j * block_rows
                accs[w, c, j] = acc[first : first + block_rows, :]
        for n in (1, 0):
            w = lax.rem(wave_me + n, WAVES)
            for i in range(heads // 2):
                remote(
                    accs.at[w, c, 2 * i + 1 - core_me],
                    pair.at[w, c, i],
                    a_send.at[w, c],
                    a_recv.at[w, c],
                    (t_me + 1 - 2 * core_me, b_me),
                )

    def pass_on(n, c):
        w = lax.rem(wave_me + n, WAVES)
        drain(pair.at[w, c], a_recv.at[w, c])
        per = quads * deep
        for i in range(heads // 2):
            both = accs[w, c, 2 * i + core_me] + pair[w, c, i]
            for g in range(per):
                psend[w, c, i * per + g] = both[g * seqs : (g + 1) * seqs, :].astype(jnp.bfloat16)

        def index(t, d):
            return lax.div(lax.rem(t, heads), 2) * per + lax.div(t, heads) * deep + d

        for mt, mb in dest_masks:

            def send(mt=mt, mb=mb):
                remote(
                    psend.at[w, c, index(t_flips[mt], deep_flips[mb])],
                    pslot.at[c, chip_me],
                    p_send.at[c],
                    p_recv.at[c],
                    (t_flips[mt], w * deep + deep_flips[mb]),
                )

            if n or mt or mb:
                send()
            else:
                pslot[c, chip_me] = psend[w, c, index(t_me, deep_me)]

    for w in range(WAVES):
        weigh(w)
    for copy in v_copies:
        copy.wait()
    for c in range(chunks + 1):
        if c < chunks:
            multiply(c)
        if c > 0:
            for n in (1, 0):
                pass_on(n, c - 1)

    for c in range(chunks):
        drain(pslot.at[c, pl.ds(0, chips - 1)], p_recv.at[c])
        total = jnp.zeros((seqs, piece), jnp.float32)
        for slot in range(chips):
            total = total + pslot[c, slot].astype(jnp.float32)
        out_ref[:, pl.ds(c * piece, piece)] = total.astype(jnp.bfloat16)

    drain_count(central, lambda n: qslot.at[pl.ds(0, n)], heads, q_send)
    drain_count(central, lambda n: kslot.at[pl.ds(0, n)], 2 * nt, k_send)
    drain(islot.at[pl.ds(0, devices - 1)], i_send)

    @pl.when(central)
    def _():
        drain(wacc.at[pl.ds(0, (devices - 1) * span // 2)], w_send)

    for c in range(chunks):
        drain(pslot.at[c, pl.ds(0, chips - 1)], p_send.at[c])
        for w in range(WAVES):
            drain(pair.at[w, c], a_send.at[w, c])


def shards(nt, nb, queries, indices, first_keys, second_keys, values):
    seqs, heads, top = indices.shape
    width_q = queries.shape[2]
    half = width_q // 2
    firsts = first_keys.shape[1]
    sub_count = second_keys.shape[1]
    rows, width = values.shape
    devices = nt * nb
    all_seqs = devices * seqs
    deep = nb // WAVES
    quads = nt // heads
    span = deep * seqs
    assert heads * top == LANES and nt % heads == 0 and heads % 2 == 0
    assert nb % WAVES == 0 and span % 8 == 0
    chunks, pieces = 2, 4
    early = all_seqs <= 256
    held = all_seqs if early else 1
    piece = width // chunks
    per_pair = (heads // 2) * quads * deep
    hbm = pl.BlockSpec(memory_space=pltpu.MemorySpace.HBM)
    dma = pltpu.SemaphoreType.DMA
    return pl.pallas_call(
        functools.partial(kernel, (nt, nb, heads, seqs, top, chunks, pieces, early)),
        out_shape=pltpu.VMEM((seqs, width), jnp.bfloat16),
        in_specs=[hbm] * 5,
        out_specs=pl.BlockSpec(memory_space=pltpu.VMEM),
        scratch_shapes=[
            pltpu.VMEM(queries.shape, queries.dtype),
            pltpu.VMEM(indices.shape, indices.dtype),
            pltpu.VMEM(first_keys.shape, first_keys.dtype),
            pltpu.VMEM((rows, width), jnp.bfloat16),
            pltpu.VMEM((sub_count, half), jnp.bfloat16),
            pltpu.VMEM((devices, firsts, half), jnp.bfloat16),
            pltpu.VMEM((devices, seqs, LANES), jnp.int32),
            pltpu.VMEM((seqs, LANES), jnp.int32),
            pltpu.VMEM((heads, seqs, width_q), jnp.float32),
            pltpu.VMEM((heads, seqs, width_q), jnp.bfloat16),
            pltpu.VMEM((heads * deep, seqs, width_q), jnp.bfloat16),
            pltpu.VMEM((heads * span, width_q), jnp.float32),
            pltpu.VMEM((span, LANES), jnp.bfloat16),
            pltpu.VMEM((WAVES * heads * quads, span, LANES), jnp.bfloat16),
            pltpu.VMEM((all_seqs, LANES), jnp.int32),
            pltpu.VMEM((all_seqs, LANES), jnp.float32),
            pltpu.VMEM((rows // LANES * (all_seqs + 8), LANES), jnp.float32),
            pltpu.VMEM((all_seqs, rows), jnp.bfloat16),
            pltpu.VMEM((held, rows // LANES, LANES), jnp.bfloat16),
            pltpu.VMEM((held, LANES, LANES), jnp.bfloat16),
            pltpu.VMEM((WAVES, chunks, heads, quads * span, piece), jnp.float32),
            pltpu.VMEM((WAVES, chunks, heads // 2, quads * span, piece), jnp.float32),
            pltpu.VMEM((WAVES, chunks, per_pair, seqs, piece), jnp.bfloat16),
            pltpu.VMEM((chunks, devices // 2, seqs, piece), jnp.bfloat16),
            pltpu.SemaphoreType.REGULAR((nb,)),
            dma((3,)),
            dma((pieces,)),
            dma,
            dma,
            dma,
            dma,
            dma((WAVES,)),
            dma,
            dma,
            dma,
            dma((WAVES,)),
            dma((WAVES, chunks)),
            dma((WAVES, chunks)),
            dma((chunks,)),
            dma((chunks,)),
        ],
        compiler_params=pltpu.CompilerParams(
            collective_id=0, has_side_effects=True, vmem_limit_bytes=56 * 1024 * 1024
        ),
    )(queries, indices, first_keys, second_keys, values)


def solution(mesh):
    placed = (
        P(("table", "batch"), None, None),
        P(("table", "batch"), None, None),
        P(None, ("table", "batch"), None),
        P(),
        P(("table", "batch"), None),
    )
    body = functools.partial(shards, mesh.shape["table"], mesh.shape["batch"])
    return jax.shard_map(
        body, mesh=mesh, in_specs=placed, out_specs=P(("table", "batch"), None), check_vma=False
    )
```

```python
import functools

import jax
import jax.numpy as jnp
from jax import lax
from jax.experimental import pallas as pl
from jax.experimental.pallas import tpu as pltpu
from jax.sharding import PartitionSpec as P

MESH = pl.DeviceIdType.MESH
LANES = 128
NT = (((1,), (1,)), ((), ()))
NN = (((1,), (0,)), ((), ()))
WAVES = 2
GROUP = 32


def log2(number):
    assert number & (number - 1) == 0
    return number.bit_length() - 1


def pick_lanes(table, ids):
    picked = jnp.zeros(ids.shape, jnp.float32)
    inner = ids & (LANES - 1)
    outer = lax.shift_right_arithmetic(ids, 7)
    for part in range(table.shape[1] // LANES):
        got = jnp.take_along_axis(table[:, part * LANES : (part + 1) * LANES], inner, axis=1)
        picked = jnp.where(outer == part, got, picked)
    return picked


def kernel(
    shape,
    q_hbm,
    i_hbm,
    fk_hbm,
    sk_hbm,
    v_hbm,
    out_ref,
    q_ref,
    i_ref,
    fk_ref,
    vbuf,
    k2buf,
    kslot,
    islot,
    icomp,
    qrows,
    qsend,
    qslot,
    qstage,
    wpack,
    wslot,
    istage,
    wfin,
    wacc,
    wb,
    highs,
    lows,
    highrow,
    accs,
    pair,
    psend,
    pslot,
    ready,
    in_sem,
    v_sem,
    k2_sem,
    k_send,
    k_recv,
    i_send,
    i_recv,
    q_send,
    q_recv,
    w_send,
    w_recv,
    a_send,
    a_recv,
    p_send,
    p_recv,
):
    nt, nb, heads, seqs, top, chunks, pieces, early = shape
    devices = nt * nb
    quads = nt // heads
    deep = nb // WAVES
    middle = deep - 1
    span = deep * seqs
    block_rows = quads * span
    wave_rows = heads * block_rows
    wave_devs = nt * deep
    all_seqs = devices * seqs
    half = fk_hbm.shape[2]
    rows, width = v_hbm.shape
    high_count = rows // LANES
    pitch = all_seqs + 8
    t_me, b_me = lax.axis_index("table"), lax.axis_index("batch")
    dev_me = t_me * nb + b_me
    core_me = lax.rem(t_me, 2)
    head_me = lax.rem(t_me, heads)
    quad_me = lax.div(t_me, heads)
    wave_me = lax.div(b_me, deep)
    deep_me = lax.rem(b_me, deep)
    central = b_me == middle

    def slot_of(t, b):
        return (
            lax.div(b, deep) * wave_devs
            + (lax.rem(t, heads) * quads + lax.div(t, heads)) * deep
            + lax.rem(b, deep)
        )

    def flips(x, count):
        bits = [(x // 2**i) % 2 for i in range(log2(count))]
        return [
            x + sum((1 - 2 * bit) * 2**i for i, bit in enumerate(bits) if mask >> i & 1)
            for mask in range(count)
        ]

    slot_me = slot_of(t_me, b_me)
    t_flips = flips(t_me, nt)
    deep_flips = flips(deep_me, deep)
    t_masks = sorted(range(nt), key=lambda m: (bin(m >> 1).count("1"), m), reverse=True)

    def unless_me(mt, k, body):
        if mt:
            body()
        else:
            pl.when(b_me != k)(body)

    def drain(ref, sem):
        pltpu.make_async_copy(ref, ref, sem).wait()

    def drain_count(less, ref_of, count, sem):
        pl.when(less)(lambda: drain(ref_of(count - 1), sem))
        pl.when(jnp.logical_not(less))(lambda: drain(ref_of(count), sem))

    def remote(src, dst, send, recv, where):
        pltpu.make_async_remote_copy(
            src_ref=src,
            dst_ref=dst,
            send_sem=send,
            recv_sem=recv,
            device_id=where,
            device_id_type=MESH,
        ).start()

    barrier = pltpu.get_barrier_semaphore()

    def greet(sem, where):
        pl.semaphore_signal(sem, inc=1, device_id=where, device_id_type=MESH)

    for k in range(nb - 1, -1, -1):

        @pl.when(b_me <= k)
        def _():
            for mt in t_masks:
                unless_me(mt, k, lambda mt=mt: greet(barrier, (t_flips[mt], k)))

    in_copies = [
        pltpu.make_async_copy(src, dst, in_sem.at[n])
        for n, (src, dst) in enumerate(((fk_hbm, fk_ref), (i_hbm, i_ref), (q_hbm, q_ref)))
    ]
    for copy in in_copies:
        copy.start()
    pl.semaphore_wait(barrier, nt * (b_me + 1) - 1)
    for k in range(nb - 1):

        @pl.when(b_me > k)
        def _():
            for mt in t_masks:
                greet(ready.at[b_me], (t_flips[mt], k))

    for copy in in_copies:
        copy.wait()

    def send_keys():
        for mt in t_masks:
            unless_me(
                mt,
                middle,
                lambda mt=mt: remote(
                    fk_ref.at[lax.rem(t_flips[mt], heads)],
                    kslot.at[dev_me],
                    k_send,
                    k_recv,
                    (t_flips[mt], middle),
                ),
            )

    pl.when(b_me >= middle)(send_keys)
    k2_copy = pltpu.make_async_copy(sk_hbm.at[head_me], k2buf, k2_sem)
    k2_copy.start()
    block = rows // pieces
    v_copies = [
        pltpu.make_async_copy(
            v_hbm.at[pl.ds(p * block, block)], vbuf.at[pl.ds(p * block, block)], v_sem.at[p]
        )
        for p in range(pieces)
    ]
    for copy in v_copies:
        copy.start()

    for h in range(heads):
        for s in range(seqs):
            icomp[pl.ds(s, 1), pl.ds(h * top, top)] = i_ref[s, pl.ds(h, 1), :]
    islot[slot_me] = icomp[...]
    kslot[dev_me] = fk_ref[head_me]
    for s in range(seqs):
        one = q_ref[s].astype(jnp.float32)
        for h in range(heads):
            qrows[h, pl.ds(s, 1), :] = one[h : h + 1, :]
    for h in range(heads):
        qsend[h] = qrows[h].astype(jnp.bfloat16)
    place_me = (wave_me * heads + head_me) * deep + deep_me
    qslot[place_me] = qsend[head_me]

    for k in (middle, *(k for k in range(nb) if k != middle)):

        @pl.when(b_me < k)
        def _():
            pl.semaphore_wait(ready.at[k], nt)

        if k == middle:
            pl.when(b_me < middle)(send_keys)
            for h in range(heads):

                @pl.when(jnp.logical_not(jnp.logical_and(central, head_me == h)))
                def _():
                    remote(
                        qsend.at[h], qslot.at[place_me], q_send, q_recv, (quad_me * heads + h, k)
                    )

        for mt in t_masks:
            unless_me(
                mt,
                k,
                lambda mt=mt, k=k: remote(
                    icomp, islot.at[slot_me], i_send, i_recv, (t_flips[mt], k)
                ),
            )

    drain(islot.at[pl.ds(0, devices - 1)], i_recv)
    for slot in range(devices):
        istage[pl.ds(slot * seqs, seqs), :] = islot[slot]
    k2_copy.wait()

    @pl.when(central)
    def _():
        places = WAVES * heads * deep
        drain(qslot.at[pl.ds(0, places - 1)], q_recv)
        for n in range(places):
            qstage[pl.ds(n * seqs, seqs), :] = qslot[n].astype(jnp.float32)
        q_all = qstage[...].astype(jnp.bfloat16)
        s2 = lax.dot_general(q_all[:, half:], k2buf[...], NT, preferred_element_type=jnp.float32)
        ids = jnp.concatenate(
            [
                istage[
                    pl.ds(pl.multiple_of(w * wave_rows + j * block_rows + quad_me * span, 8), span),
                    :,
                ]
                for w in range(WAVES)
                for j in range(heads)
            ],
            axis=0,
        )
        sub_count = k2buf.shape[0]
        second = pick_lanes(s2, ids & (sub_count - 1))
        drain(kslot.at[pl.ds(0, devices - 1)], k_recv)
        k1 = kslot[...].astype(jnp.float32)
        k1 = k1.reshape(k1.shape[0] * k1.shape[1], half).astype(jnp.bfloat16)
        s1 = lax.dot_general(q_all[:, :half], k1, NT, preferred_element_type=jnp.float32)
        score = second + pick_lanes(s1, lax.shift_right_arithmetic(ids, log2(sub_count)))
        lane = lax.broadcasted_iota(jnp.int32, ids.shape, 1)
        mine = lax.shift_right_arithmetic(lane, log2(top)) == head_me
        best = jnp.max(jnp.where(mine, score, -jnp.inf), axis=1, keepdims=True)
        raised = jnp.where(mine, jnp.exp(jnp.where(mine, score - best, 0.0)), 0.0)
        weights = raised / jnp.sum(raised, axis=1, keepdims=True)
        weights = weights.astype(jnp.bfloat16).astype(jnp.float32)
        for w in range(WAVES):
            packed = jnp.zeros((span, LANES), jnp.float32)
            for j in range(heads):
                first = (w * heads + j) * span
                packed = packed + pltpu.roll(
                    weights[first : first + span, :],
                    lax.rem(j - head_me + heads, heads) * top,
                    1,
                )
            wpack[pl.ds(w * span, span), :] = packed.astype(jnp.bfloat16)
        where_me = head_me * quads + quad_me
        wslot[where_me] = wpack[...]
        for k in sorted(range(nb), key=lambda k: abs(k - middle), reverse=True):
            for mt in t_masks:
                unless_me(
                    mt,
                    k,
                    lambda mt=mt, k=k: remote(
                        wpack, wslot.at[where_me], w_send, w_recv, (t_flips[mt], k)
                    ),
                )

    high_iota = lax.broadcasted_iota(jnp.int32, (high_count, LANES), 0)
    low_iota = lax.broadcasted_iota(jnp.int32, (LANES, LANES), 0)
    high_hot = high_iota.astype(jnp.float32).astype(jnp.bfloat16)
    low_lane = lax.broadcasted_iota(jnp.int32, (LANES, LANES), 1)
    low_lane = low_lane.astype(jnp.float32).astype(jnp.bfloat16)
    base = dev_me * rows
    one, zero = jnp.bfloat16(1.0), jnp.bfloat16(0.0)

    def build_masks():
        entries = istage[...]
        highrow[...] = lax.shift_right_arithmetic(entries - base, 7).astype(jnp.float32)

        def build(step, carry):
            first = pl.multiple_of(step * GROUP, GROUP)
            some = (istage[pl.ds(first, GROUP), :] & (LANES - 1)).astype(jnp.float32).T
            for u in range(GROUP):
                column = jnp.broadcast_to(some[:, u : u + 1], (LANES, LANES))
                lows[first + u] = jnp.where(low_lane == column.astype(jnp.bfloat16), one, zero)
                row = jnp.broadcast_to(highrow[pl.ds(first + u, 1), :], (high_count, LANES))
                highs[first + u] = jnp.where(high_hot == row.astype(jnp.bfloat16), one, zero)
            return carry

        lax.fori_loop(0, all_seqs // GROUP, build, 0)

    if early:
        build_masks()

    piece = width // chunks
    chip_me = lax.div(t_me, 2) * nb + b_me
    chips = devices // 2
    lane = lax.broadcasted_iota(jnp.int32, (block_rows, LANES), 1)
    block_of = lax.shift_right_arithmetic(lane, log2(top))
    dest_masks = sorted(
        ((mt, mb) for mt in range(0, nt, 2) for mb in range(deep)),
        key=lambda m: (bin(m[0] >> 1).count("1") + m[1], m),
        reverse=True,
    )

    def weigh():
        drain_count(central, lambda n: wslot.at[pl.ds(0, n)], heads * quads, w_recv)
        for w in range(WAVES):
            parts = [
                wslot[pl.ds(h * quads, quads), pl.ds(w * span, span), :]
                .astype(jnp.float32)
                .reshape(block_rows, LANES)
                for h in range(heads)
            ]
            for j in range(heads):
                total = jnp.zeros((block_rows, LANES), jnp.float32)
                for h in range(heads):
                    part = parts[h]
                    if h != j:
                        part = pltpu.roll(part, (h - j) % heads * top, 1)
                    total = jnp.where(block_of == h, part, total)
                wfin[pl.ds(w * wave_rows + j * block_rows, block_rows), :] = total

        def spread(step, carry):
            for u in range(32):
                s = step * 32 + u
                weight = wfin[pl.ds(s, 1), :]
                if early:
                    left = highs[s] * jnp.broadcast_to(weight, (high_count, LANES)).astype(
                        jnp.bfloat16
                    )
                    got = lax.dot_general(left, lows[s], NN, preferred_element_type=jnp.float32)
                else:
                    row = istage[pl.ds(s, 1), :]
                    high = lax.shift_right_arithmetic(row - base, 7)
                    left = jnp.where(high_iota == high, weight, 0.0).astype(jnp.bfloat16)
                    low = jnp.where(low_iota == (row & (LANES - 1)), 1.0, 0.0)
                    got = lax.dot_general(
                        left, low.astype(jnp.bfloat16), NT, preferred_element_type=jnp.float32
                    )
                wacc[pl.ds(s, high_count, stride=pitch), :] = got
            return carry

        lax.fori_loop(0, all_seqs // 32, spread, 0)

        def narrow(step, carry):
            wb[:, pl.ds(pl.multiple_of(step * LANES, LANES), LANES)] = wacc[
                pl.ds(pl.multiple_of(step * pitch, 8), all_seqs), :
            ].astype(jnp.bfloat16)
            return carry

        lax.fori_loop(0, high_count, narrow, 0, unroll=8)

    def multiply(c):
        acc = jnp.dot(
            wb[...], vbuf[:, pl.ds(c * piece, piece)], preferred_element_type=jnp.float32
        )
        for w in range(WAVES):
            for j in range(heads):
                first = w * wave_rows + j * block_rows
                accs[w, c, j] = acc[first : first + block_rows, :]
        for n in (1, 0):
            w = lax.rem(wave_me + n, WAVES)
            for i in range(heads // 2):
                remote(
                    accs.at[w, c, 2 * i + 1 - core_me],
                    pair.at[w, c, i],
                    a_send.at[w, c],
                    a_recv.at[w, c],
                    (t_me + 1 - 2 * core_me, b_me),
                )

    def pass_on(n, c):
        w = lax.rem(wave_me + n, WAVES)
        drain(pair.at[w, c], a_recv.at[w, c])
        per = quads * deep
        for i in range(heads // 2):
            both = accs[w, c, 2 * i + core_me] + pair[w, c, i]
            for g in range(per):
                psend[w, c, i * per + g] = both[g * seqs : (g + 1) * seqs, :].astype(jnp.bfloat16)

        def index(t, d):
            return lax.div(lax.rem(t, heads), 2) * per + lax.div(t, heads) * deep + d

        for mt, mb in dest_masks:

            def send(mt=mt, mb=mb):
                remote(
                    psend.at[w, c, index(t_flips[mt], deep_flips[mb])],
                    pslot.at[c, chip_me],
                    p_send.at[c],
                    p_recv.at[c],
                    (t_flips[mt], w * deep + deep_flips[mb]),
                )

            if n or mt or mb:
                send()
            else:
                pslot[c, chip_me] = psend[w, c, index(t_me, deep_me)]

    weigh()
    for copy in v_copies:
        copy.wait()
    for c in range(chunks + 1):
        if c < chunks:
            multiply(c)
        if c > 0:
            for n in (1, 0):
                pass_on(n, c - 1)

    for c in range(chunks):
        drain(pslot.at[c, pl.ds(0, chips - 1)], p_recv.at[c])
        total = jnp.zeros((seqs, piece), jnp.float32)
        for slot in range(chips):
            total = total + pslot[c, slot].astype(jnp.float32)
        out_ref[:, pl.ds(c * piece, piece)] = total.astype(jnp.bfloat16)

    drain_count(central, lambda n: qslot.at[pl.ds(0, n)], heads, q_send)
    drain_count(central, lambda n: kslot.at[pl.ds(0, n)], nt, k_send)
    drain(islot.at[pl.ds(0, devices - 1)], i_send)

    @pl.when(central)
    def _():
        drain(wacc.at[pl.ds(0, (devices - 1) * WAVES * span // 2)], w_send)

    for c in range(chunks):
        drain(pslot.at[c, pl.ds(0, chips - 1)], p_send.at[c])
        for w in range(WAVES):
            drain(pair.at[w, c], a_send.at[w, c])


def shards(nt, nb, queries, indices, first_keys, second_keys, values):
    seqs, heads, top = indices.shape
    width_q = queries.shape[2]
    half = width_q // 2
    firsts = first_keys.shape[1]
    sub_count = second_keys.shape[1]
    rows, width = values.shape
    devices = nt * nb
    all_seqs = devices * seqs
    deep = nb // WAVES
    quads = nt // heads
    span = deep * seqs
    assert heads * top == LANES and nt % heads == 0 and heads % 2 == 0
    assert nb % WAVES == 0 and span % 8 == 0
    chunks, pieces = 2, 4
    early = all_seqs <= 256
    held = all_seqs if early else 1
    piece = width // chunks
    per_pair = (heads // 2) * quads * deep
    hbm = pl.BlockSpec(memory_space=pltpu.MemorySpace.HBM)
    dma = pltpu.SemaphoreType.DMA
    return pl.pallas_call(
        functools.partial(kernel, (nt, nb, heads, seqs, top, chunks, pieces, early)),
        out_shape=pltpu.VMEM((seqs, width), jnp.bfloat16),
        in_specs=[hbm] * 5,
        out_specs=pl.BlockSpec(memory_space=pltpu.VMEM),
        scratch_shapes=[
            pltpu.VMEM(queries.shape, queries.dtype),
            pltpu.VMEM(indices.shape, indices.dtype),
            pltpu.VMEM(first_keys.shape, first_keys.dtype),
            pltpu.VMEM((rows, width), jnp.bfloat16),
            pltpu.VMEM((sub_count, half), jnp.bfloat16),
            pltpu.VMEM((devices, firsts, half), jnp.bfloat16),
            pltpu.VMEM((devices, seqs, LANES), jnp.int32),
            pltpu.VMEM((seqs, LANES), jnp.int32),
            pltpu.VMEM((heads, seqs, width_q), jnp.float32),
            pltpu.VMEM((heads, seqs, width_q), jnp.bfloat16),
            pltpu.VMEM((heads * nb, seqs, width_q), jnp.bfloat16),
            pltpu.VMEM((heads * nb * seqs, width_q), jnp.float32),
            pltpu.VMEM((WAVES * span, LANES), jnp.bfloat16),
            pltpu.VMEM((heads * quads, WAVES * span, LANES), jnp.bfloat16),
            pltpu.VMEM((all_seqs, LANES), jnp.int32),
            pltpu.VMEM((all_seqs, LANES), jnp.float32),
            pltpu.VMEM((rows // LANES * (all_seqs + 8), LANES), jnp.float32),
            pltpu.VMEM((all_seqs, rows), jnp.bfloat16),
            pltpu.VMEM((held, rows // LANES, LANES), jnp.bfloat16),
            pltpu.VMEM((held, LANES, LANES), jnp.bfloat16),
            pltpu.VMEM((all_seqs, LANES), jnp.float32),
            pltpu.VMEM((WAVES, chunks, heads, quads * span, piece), jnp.float32),
            pltpu.VMEM((WAVES, chunks, heads // 2, quads * span, piece), jnp.float32),
            pltpu.VMEM((WAVES, chunks, per_pair, seqs, piece), jnp.bfloat16),
            pltpu.VMEM((chunks, devices // 2, seqs, piece), jnp.bfloat16),
            pltpu.SemaphoreType.REGULAR((nb,)),
            dma((3,)),
            dma((pieces,)),
            dma,
            dma,
            dma,
            dma,
            dma,
            dma,
            dma,
            dma,
            dma,
            dma((WAVES, chunks)),
            dma((WAVES, chunks)),
            dma((chunks,)),
            dma((chunks,)),
        ],
        compiler_params=pltpu.CompilerParams(
            collective_id=0, has_side_effects=True, vmem_limit_bytes=56 * 1024 * 1024
        ),
    )(queries, indices, first_keys, second_keys, values)


def solution(mesh):
    placed = (
        P(("table", "batch"), None, None),
        P(("table", "batch"), None, None),
        P(None, ("table", "batch"), None),
        P(),
        P(("table", "batch"), None),
    )
    body = functools.partial(shards, mesh.shape["table"], mesh.shape["batch"])
    return jax.shard_map(
        body, mesh=mesh, in_specs=placed, out_specs=P(("table", "batch"), None), check_vma=False
    )
```

```python
import functools

import jax
import jax.numpy as jnp
from jax import lax
from jax.experimental import pallas as pl
from jax.experimental.pallas import tpu as pltpu
from jax.sharding import PartitionSpec as P

MESH = pl.DeviceIdType.MESH
LANES = 128
NT = (((1,), (1,)), ((), ()))
NN = (((1,), (0,)), ((), ()))
WAVES = 2
GROUP = 32


def log2(number):
    assert number & (number - 1) == 0
    return number.bit_length() - 1


def pick_lanes(table, ids):
    picked = jnp.zeros(ids.shape, jnp.float32)
    inner = ids & (LANES - 1)
    outer = lax.shift_right_arithmetic(ids, 7)
    for part in range(table.shape[1] // LANES):
        got = jnp.take_along_axis(table[:, part * LANES : (part + 1) * LANES], inner, axis=1)
        picked = jnp.where(outer == part, got, picked)
    return picked


def kernel(
    shape,
    q_hbm,
    i_hbm,
    fk_hbm,
    sk_hbm,
    v_hbm,
    out_ref,
    q_ref,
    i_ref,
    fk_ref,
    vbuf,
    k2buf,
    kslot,
    islot,
    icomp,
    qrows,
    qsend,
    qslot,
    qstage,
    wpack,
    wslot,
    istage,
    wfin,
    wacc,
    wb,
    highs,
    lows,
    highrow,
    accs,
    pair,
    psend,
    pslot,
    ready,
    in_sem,
    v_sem,
    k2_sem,
    k_send,
    k_recv,
    i_send,
    i_recv,
    q_send,
    q_recv,
    w_send,
    w_recv,
    a_send,
    a_recv,
    p_send,
    p_recv,
):
    nt, nb, heads, seqs, top, chunks, pieces, early = shape
    devices = nt * nb
    quads = nt // heads
    deep = nb // WAVES
    middle = deep - 1
    span = deep * seqs
    block_rows = quads * span
    wave_rows = heads * block_rows
    wave_devs = nt * deep
    all_seqs = devices * seqs
    half = fk_hbm.shape[2]
    rows, width = v_hbm.shape
    high_count = rows // LANES
    pitch = all_seqs + 4
    t_me, b_me = lax.axis_index("table"), lax.axis_index("batch")
    dev_me = t_me * nb + b_me
    core_me = lax.rem(t_me, 2)
    head_me = lax.rem(t_me, heads)
    quad_me = lax.div(t_me, heads)
    wave_me = lax.div(b_me, deep)
    deep_me = lax.rem(b_me, deep)
    central = b_me == middle

    def slot_of(t, b):
        return (
            lax.div(b, deep) * wave_devs
            + (lax.rem(t, heads) * quads + lax.div(t, heads)) * deep
            + lax.rem(b, deep)
        )

    def flips(x, count):
        bits = [(x // 2**i) % 2 for i in range(log2(count))]
        return [
            x + sum((1 - 2 * bit) * 2**i for i, bit in enumerate(bits) if mask >> i & 1)
            for mask in range(count)
        ]

    slot_me = slot_of(t_me, b_me)
    t_flips = flips(t_me, nt)
    t_masks = sorted(range(nt), key=lambda m: (bin(m >> 1).count("1"), m), reverse=True)

    def unless_me(mt, k, body):
        if mt:
            body()
        else:
            pl.when(b_me != k)(body)

    def drain(ref, sem):
        pltpu.make_async_copy(ref, ref, sem).wait()

    def drain_count(less, ref_of, count, sem):
        pl.when(less)(lambda: drain(ref_of(count - 1), sem))
        pl.when(jnp.logical_not(less))(lambda: drain(ref_of(count), sem))

    def remote(src, dst, send, recv, where):
        pltpu.make_async_remote_copy(
            src_ref=src,
            dst_ref=dst,
            send_sem=send,
            recv_sem=recv,
            device_id=where,
            device_id_type=MESH,
        ).start()

    in_copies = [
        pltpu.make_async_copy(src, dst, in_sem.at[n])
        for n, (src, dst) in enumerate(((fk_hbm, fk_ref), (i_hbm, i_ref), (q_hbm, q_ref)))
    ]
    for copy in in_copies:
        copy.start()
    barrier = pltpu.get_barrier_semaphore()

    def greet(sem, where):
        pl.semaphore_signal(sem, inc=1, device_id=where, device_id_type=MESH)

    for k in range(nb - 1, -1, -1):

        @pl.when(b_me <= k)
        def _():
            for mt in t_masks:
                unless_me(mt, k, lambda mt=mt: greet(barrier, (t_flips[mt], k)))

    pl.semaphore_wait(barrier, nt * (b_me + 1) - 1)
    for k in range(nb - 1):

        @pl.when(b_me > k)
        def _():
            for mt in t_masks:
                greet(ready.at[b_me], (t_flips[mt], k))

    for copy in in_copies:
        copy.wait()

    def send_keys():
        for mt in t_masks:
            unless_me(
                mt,
                middle,
                lambda mt=mt: remote(
                    fk_ref.at[lax.rem(t_flips[mt], heads)],
                    kslot.at[dev_me],
                    k_send,
                    k_recv,
                    (t_flips[mt], middle),
                ),
            )

    pl.when(b_me >= middle)(send_keys)
    k2_copy = pltpu.make_async_copy(sk_hbm.at[head_me], k2buf, k2_sem)
    k2_copy.start()
    block = rows // pieces
    v_copies = [
        pltpu.make_async_copy(
            v_hbm.at[pl.ds(p * block, block)], vbuf.at[pl.ds(p * block, block)], v_sem.at[p]
        )
        for p in range(pieces)
    ]
    for copy in v_copies:
        copy.start()

    for h in range(heads):
        for s in range(seqs):
            icomp[pl.ds(s, 1), pl.ds(h * top, top)] = i_ref[s, pl.ds(h, 1), :]
    islot[slot_me] = icomp[...]
    kslot[dev_me] = fk_ref[head_me]
    for s in range(seqs):
        one = q_ref[s].astype(jnp.float32)
        for h in range(heads):
            qrows[h, pl.ds(s, 1), :] = one[h : h + 1, :]
    for h in range(heads):
        qsend[h] = qrows[h].astype(jnp.bfloat16)
    place_me = (wave_me * heads + head_me) * deep + deep_me
    qslot[place_me] = qsend[head_me]

    for k in (middle, *(k for k in range(nb) if k != middle)):

        @pl.when(b_me < k)
        def _():
            pl.semaphore_wait(ready.at[k], nt)

        if k == middle:
            pl.when(b_me < middle)(send_keys)
            for h in range(heads):

                @pl.when(jnp.logical_not(jnp.logical_and(central, head_me == h)))
                def _():
                    remote(
                        qsend.at[h], qslot.at[place_me], q_send, q_recv, (quad_me * heads + h, k)
                    )

        for mt in t_masks:
            unless_me(
                mt,
                k,
                lambda mt=mt, k=k: remote(
                    icomp, islot.at[slot_me], i_send, i_recv, (t_flips[mt], k)
                ),
            )

    drain(islot.at[pl.ds(0, devices - 1)], i_recv)
    for slot in range(devices):
        istage[pl.ds(slot * seqs, seqs), :] = islot[slot]
    k2_copy.wait()

    @pl.when(central)
    def _():
        places = WAVES * heads * deep
        drain(qslot.at[pl.ds(0, places - 1)], q_recv)
        for n in range(places):
            qstage[pl.ds(n * seqs, seqs), :] = qslot[n].astype(jnp.float32)
        q_all = qstage[...].astype(jnp.bfloat16)
        s2 = lax.dot_general(q_all[:, half:], k2buf[...], NT, preferred_element_type=jnp.float32)
        ids = jnp.concatenate(
            [
                istage[
                    pl.ds(pl.multiple_of(w * wave_rows + j * block_rows + quad_me * span, 8), span),
                    :,
                ]
                for w in range(WAVES)
                for j in range(heads)
            ],
            axis=0,
        )
        sub_count = k2buf.shape[0]
        second = pick_lanes(s2, ids & (sub_count - 1))
        drain(kslot.at[pl.ds(0, devices - 1)], k_recv)
        k1 = kslot[...].astype(jnp.float32)
        k1 = k1.reshape(k1.shape[0] * k1.shape[1], half).astype(jnp.bfloat16)
        s1 = lax.dot_general(q_all[:, :half], k1, NT, preferred_element_type=jnp.float32)
        score = second + pick_lanes(s1, lax.shift_right_arithmetic(ids, log2(sub_count)))
        lane = lax.broadcasted_iota(jnp.int32, ids.shape, 1)
        mine = lax.shift_right_arithmetic(lane, log2(top)) == head_me
        best = jnp.max(jnp.where(mine, score, -jnp.inf), axis=1, keepdims=True)
        raised = jnp.where(mine, jnp.exp(jnp.where(mine, score - best, 0.0)), 0.0)
        weights = raised / jnp.sum(raised, axis=1, keepdims=True)
        weights = weights.astype(jnp.bfloat16).astype(jnp.float32)
        for w in range(WAVES):
            packed = jnp.zeros((span, LANES), jnp.float32)
            for j in range(heads):
                first = (w * heads + j) * span
                packed = packed + pltpu.roll(
                    weights[first : first + span, :],
                    lax.rem(j - head_me + heads, heads) * top,
                    1,
                )
            wpack[pl.ds(w * span, span), :] = packed.astype(jnp.bfloat16)
        where_me = head_me * quads + quad_me
        wslot[where_me] = wpack[...]
        for k in sorted(range(nb), key=lambda k: abs(k - middle), reverse=True):
            for mt in t_masks:
                unless_me(
                    mt,
                    k,
                    lambda mt=mt, k=k: remote(
                        wpack, wslot.at[where_me], w_send, w_recv, (t_flips[mt], k)
                    ),
                )

    high_iota = lax.broadcasted_iota(jnp.int32, (high_count, LANES), 0)
    low_iota = lax.broadcasted_iota(jnp.int32, (LANES, LANES), 0)
    high_hot = high_iota.astype(jnp.float32).astype(jnp.bfloat16)
    low_lane = lax.broadcasted_iota(jnp.int32, (LANES, LANES), 1)
    low_lane = low_lane.astype(jnp.float32).astype(jnp.bfloat16)
    base = dev_me * rows
    one, zero = jnp.bfloat16(1.0), jnp.bfloat16(0.0)

    def build_masks():
        entries = istage[...]
        highrow[...] = lax.shift_right_arithmetic(entries - base, 7).astype(jnp.float32)

        def build(step, carry):
            first = pl.multiple_of(step * GROUP, GROUP)
            some = (istage[pl.ds(first, GROUP), :] & (LANES - 1)).astype(jnp.float32).T
            for u in range(GROUP):
                column = jnp.broadcast_to(some[:, u : u + 1], (LANES, LANES))
                lows[first + u] = jnp.where(low_lane == column.astype(jnp.bfloat16), one, zero)
                row = jnp.broadcast_to(highrow[pl.ds(first + u, 1), :], (high_count, LANES))
                highs[first + u] = jnp.where(high_hot == row.astype(jnp.bfloat16), one, zero)
            return carry

        lax.fori_loop(0, all_seqs // GROUP, build, 0)

    if early:
        build_masks()

    piece = width // chunks
    chip_me = lax.div(t_me, 2) * nb + b_me
    chips = devices // 2
    lane = lax.broadcasted_iota(jnp.int32, (block_rows, LANES), 1)
    block_of = lax.shift_right_arithmetic(lane, log2(top))
    def weigh():
        drain_count(central, lambda n: wslot.at[pl.ds(0, n)], heads * quads, w_recv)
        for w in range(WAVES):
            parts = [
                wslot[pl.ds(h * quads, quads), pl.ds(w * span, span), :]
                .astype(jnp.float32)
                .reshape(block_rows, LANES)
                for h in range(heads)
            ]
            for j in range(heads):
                total = jnp.zeros((block_rows, LANES), jnp.float32)
                for h in range(heads):
                    part = parts[h]
                    if h != j:
                        part = pltpu.roll(part, (h - j) % heads * top, 1)
                    total = jnp.where(block_of == h, part, total)
                wfin[pl.ds(w * wave_rows + j * block_rows, block_rows), :] = total

        def spread(step, carry):
            for u in range(128):
                s = step * 128 + u
                weight = wfin[pl.ds(s, 1), :]
                if early:
                    left = highs[s] * jnp.broadcast_to(weight, (high_count, LANES)).astype(
                        jnp.bfloat16
                    )
                    got = lax.dot_general(left, lows[s], NN, preferred_element_type=jnp.float32)
                else:
                    row = istage[pl.ds(s, 1), :]
                    high = lax.shift_right_arithmetic(row - base, 7)
                    left = jnp.where(high_iota == high, weight, 0.0).astype(jnp.bfloat16)
                    low = jnp.where(low_iota == (row & (LANES - 1)), 1.0, 0.0)
                    got = lax.dot_general(
                        left, low.astype(jnp.bfloat16), NT, preferred_element_type=jnp.float32
                    )
                wacc[pl.ds(s, high_count, stride=pitch), :] = got
            return carry

        lax.fori_loop(0, all_seqs // 128, spread, 0)

        for step in range(high_count):
            wb[:, pl.ds(step * LANES, LANES)] = wacc[pl.ds(step * pitch, all_seqs), :].astype(
                jnp.bfloat16
            )

    def multiply(c):
        acc = jnp.dot(
            wb[...], vbuf[:, pl.ds(c * piece, piece)], preferred_element_type=jnp.float32
        )
        for w in range(WAVES):
            for j in range(heads):
                first = w * wave_rows + j * block_rows
                accs[w, c, j] = acc[first : first + block_rows, :]
        for w in range(WAVES):
            for i in range(heads // 2):
                remote(
                    accs.at[w, c, 2 * i + 1 - core_me],
                    pair.at[w, c, i],
                    a_send.at[w, c],
                    a_recv.at[w, c],
                    (t_me + 1 - 2 * core_me, b_me),
                )

    def pass_on(w, c):
        drain(pair.at[w, c], a_recv.at[w, c])
        per = quads * deep
        for i in range(heads // 2):
            both = accs[w, c, 2 * i + core_me] + pair[w, c, i]
            for g in range(per):
                psend[w, c, i * per + g] = both[g * seqs : (g + 1) * seqs, :].astype(jnp.bfloat16)
        for d in range(deep):
            for chip in range(nt // 2):
                k = w * deep + d
                place = chip % (heads // 2) * per + chip // (heads // 2) * deep + d
                mine = jnp.logical_and(lax.div(t_me, 2) == chip, b_me == k)

                @pl.when(jnp.logical_not(mine))
                def _():
                    remote(
                        psend.at[w, c, place],
                        pslot.at[c, chip_me],
                        p_send.at[c],
                        p_recv.at[c],
                        (2 * chip + core_me, k),
                    )

                @pl.when(mine)
                def _():
                    pslot[c, chip_me] = psend[w, c, place]

    for copy in v_copies:
        copy.wait()
    weigh()
    for c in range(chunks + 1):
        if c < chunks:
            multiply(c)
        if c > 0:
            for w in range(WAVES):
                pass_on(w, c - 1)

    for c in range(chunks):
        drain(pslot.at[c, pl.ds(0, chips - 1)], p_recv.at[c])
        total = jnp.zeros((seqs, piece), jnp.float32)
        for slot in range(chips):
            total = total + pslot[c, slot].astype(jnp.float32)
        out_ref[:, pl.ds(c * piece, piece)] = total.astype(jnp.bfloat16)

    drain_count(central, lambda n: qslot.at[pl.ds(0, n)], heads, q_send)
    drain_count(central, lambda n: kslot.at[pl.ds(0, n)], nt, k_send)
    drain(islot.at[pl.ds(0, devices - 1)], i_send)

    @pl.when(central)
    def _():
        drain(wacc.at[pl.ds(0, (devices - 1) * WAVES * span // 2)], w_send)

    for c in range(chunks):
        drain(pslot.at[c, pl.ds(0, chips - 1)], p_send.at[c])
        for w in range(WAVES):
            drain(pair.at[w, c], a_send.at[w, c])


def shards(nt, nb, queries, indices, first_keys, second_keys, values):
    seqs, heads, top = indices.shape
    width_q = queries.shape[2]
    half = width_q // 2
    firsts = first_keys.shape[1]
    sub_count = second_keys.shape[1]
    rows, width = values.shape
    devices = nt * nb
    all_seqs = devices * seqs
    deep = nb // WAVES
    quads = nt // heads
    span = deep * seqs
    assert heads * top == LANES and nt % heads == 0 and heads % 2 == 0
    assert nb % WAVES == 0 and span % 8 == 0
    chunks, pieces = 2, 4
    early = all_seqs <= 256
    held = all_seqs if early else 1
    piece = width // chunks
    per_pair = (heads // 2) * quads * deep
    hbm = pl.BlockSpec(memory_space=pltpu.MemorySpace.HBM)
    dma = pltpu.SemaphoreType.DMA
    return pl.pallas_call(
        functools.partial(kernel, (nt, nb, heads, seqs, top, chunks, pieces, early)),
        out_shape=pltpu.VMEM((seqs, width), jnp.bfloat16),
        in_specs=[hbm] * 5,
        out_specs=pl.BlockSpec(memory_space=pltpu.VMEM),
        scratch_shapes=[
            pltpu.VMEM(queries.shape, queries.dtype),
            pltpu.VMEM(indices.shape, indices.dtype),
            pltpu.VMEM(first_keys.shape, first_keys.dtype),
            pltpu.VMEM((rows, width), jnp.bfloat16),
            pltpu.VMEM((sub_count, half), jnp.bfloat16),
            pltpu.VMEM((devices, firsts, half), jnp.bfloat16),
            pltpu.VMEM((devices, seqs, LANES), jnp.int32),
            pltpu.VMEM((seqs, LANES), jnp.int32),
            pltpu.VMEM((heads, seqs, width_q), jnp.float32),
            pltpu.VMEM((heads, seqs, width_q), jnp.bfloat16),
            pltpu.VMEM((heads * nb, seqs, width_q), jnp.bfloat16),
            pltpu.VMEM((heads * nb * seqs, width_q), jnp.float32),
            pltpu.VMEM((WAVES * span, LANES), jnp.bfloat16),
            pltpu.VMEM((heads * quads, WAVES * span, LANES), jnp.bfloat16),
            pltpu.VMEM((all_seqs, LANES), jnp.int32),
            pltpu.VMEM((all_seqs, LANES), jnp.float32),
            pltpu.VMEM((rows // LANES * (all_seqs + 4), LANES), jnp.float32),
            pltpu.VMEM((all_seqs, rows), jnp.bfloat16),
            pltpu.VMEM((held, rows // LANES, LANES), jnp.bfloat16),
            pltpu.VMEM((held, LANES, LANES), jnp.bfloat16),
            pltpu.VMEM((all_seqs, LANES), jnp.float32),
            pltpu.VMEM((WAVES, chunks, heads, quads * span, piece), jnp.float32),
            pltpu.VMEM((WAVES, chunks, heads // 2, quads * span, piece), jnp.float32),
            pltpu.VMEM((WAVES, chunks, per_pair, seqs, piece), jnp.bfloat16),
            pltpu.VMEM((chunks, devices // 2, seqs, piece), jnp.bfloat16),
            pltpu.SemaphoreType.REGULAR((nb,)),
            dma((3,)),
            dma((pieces,)),
            dma,
            dma,
            dma,
            dma,
            dma,
            dma,
            dma,
            dma,
            dma,
            dma((WAVES, chunks)),
            dma((WAVES, chunks)),
            dma((chunks,)),
            dma((chunks,)),
        ],
        compiler_params=pltpu.CompilerParams(
            collective_id=0, has_side_effects=True, vmem_limit_bytes=56 * 1024 * 1024
        ),
    )(queries, indices, first_keys, second_keys, values)


def solution(mesh):
    placed = (
        P(("table", "batch"), None, None),
        P(("table", "batch"), None, None),
        P(None, ("table", "batch"), None),
        P(),
        P(("table", "batch"), None),
    )
    body = functools.partial(shards, mesh.shape["table"], mesh.shape["batch"])
    return jax.shard_map(
        body, mesh=mesh, in_specs=placed, out_specs=P(("table", "batch"), None), check_vma=False
    )
```

```python
import functools

import jax
import jax.numpy as jnp
from jax import lax
from jax.experimental import pallas as pl
from jax.experimental.pallas import tpu as pltpu
from jax.sharding import PartitionSpec as P

MESH = pl.DeviceIdType.MESH
LANES = 128
NT = (((1,), (1,)), ((), ()))
NN = (((1,), (0,)), ((), ()))
WAVES = 2
GROUP = 32
DIRECT = 1


def log2(number):
    assert number & (number - 1) == 0
    return number.bit_length() - 1


def pick_lanes(table, ids):
    picked = jnp.zeros(ids.shape, jnp.float32)
    inner = ids & (LANES - 1)
    outer = lax.shift_right_arithmetic(ids, 7)
    for part in range(table.shape[1] // LANES):
        got = jnp.take_along_axis(table[:, part * LANES : (part + 1) * LANES], inner, axis=1)
        picked = jnp.where(outer == part, got, picked)
    return picked


def kernel(
    shape,
    q_hbm,
    i_hbm,
    fk_hbm,
    sk_hbm,
    v_hbm,
    out_ref,
    q_ref,
    i_ref,
    fk_ref,
    vbuf,
    k2buf,
    kslot,
    islot,
    icomp,
    qrows,
    qsend,
    qslot,
    qstage,
    wpack,
    wslot,
    istage,
    wfin,
    wacc,
    wb,
    highs,
    lows,
    highrow,
    accs,
    pair,
    psend,
    pslot,
    dsend,
    dslot,
    ready,
    in_sem,
    v_sem,
    k2_sem,
    k_send,
    k_recv,
    i_send,
    i_recv,
    q_send,
    q_recv,
    w_send,
    w_recv,
    a_send,
    a_recv,
    p_send,
    p_recv,
    d_send,
    d_recv,
):
    nt, nb, heads, seqs, top, chunks, pieces, early = shape
    devices = nt * nb
    quads = nt // heads
    deep = nb // WAVES
    middle = deep - 1
    span = deep * seqs
    block_rows = quads * span
    wave_rows = heads * block_rows
    wave_devs = nt * deep
    all_seqs = devices * seqs
    half = fk_hbm.shape[2]
    rows, width = v_hbm.shape
    high_count = rows // LANES
    pitch = all_seqs + 4
    t_me, b_me = lax.axis_index("table"), lax.axis_index("batch")
    dev_me = t_me * nb + b_me
    core_me = lax.rem(t_me, 2)
    head_me = lax.rem(t_me, heads)
    quad_me = lax.div(t_me, heads)
    wave_me = lax.div(b_me, deep)
    deep_me = lax.rem(b_me, deep)
    central = b_me == middle
    direct = jnp.logical_and(t_me < 2 * DIRECT, b_me == 0)

    def slot_of(t, b):
        return (
            lax.div(b, deep) * wave_devs
            + (lax.rem(t, heads) * quads + lax.div(t, heads)) * deep
            + lax.rem(b, deep)
        )

    def flips(x, count):
        bits = [(x // 2**i) % 2 for i in range(log2(count))]
        return [
            x + sum((1 - 2 * bit) * 2**i for i, bit in enumerate(bits) if mask >> i & 1)
            for mask in range(count)
        ]

    slot_me = slot_of(t_me, b_me)
    t_flips = flips(t_me, nt)
    t_masks = sorted(range(nt), key=lambda m: (bin(m >> 1).count("1"), m), reverse=True)

    def unless_me(mt, k, body):
        if mt:
            body()
        else:
            pl.when(b_me != k)(body)

    def drain(ref, sem):
        pltpu.make_async_copy(ref, ref, sem).wait()

    def drain_count(less, ref_of, count, sem):
        pl.when(less)(lambda: drain(ref_of(count - 1), sem))
        pl.when(jnp.logical_not(less))(lambda: drain(ref_of(count), sem))

    def remote(src, dst, send, recv, where):
        pltpu.make_async_remote_copy(
            src_ref=src,
            dst_ref=dst,
            send_sem=send,
            recv_sem=recv,
            device_id=where,
            device_id_type=MESH,
        ).start()

    in_copies = [
        pltpu.make_async_copy(src, dst, in_sem.at[n])
        for n, (src, dst) in enumerate(((fk_hbm, fk_ref), (i_hbm, i_ref), (q_hbm, q_ref)))
    ]
    for copy in in_copies:
        copy.start()
    barrier = pltpu.get_barrier_semaphore()

    def greet(sem, where):
        pl.semaphore_signal(sem, inc=1, device_id=where, device_id_type=MESH)

    for k in range(nb - 1, -1, -1):

        @pl.when(b_me <= k)
        def _():
            for mt in t_masks:
                unless_me(mt, k, lambda mt=mt: greet(barrier, (t_flips[mt], k)))

    pl.semaphore_wait(barrier, nt * (b_me + 1) - 1)
    for k in range(nb - 1):

        @pl.when(b_me > k)
        def _():
            for mt in t_masks:
                greet(ready.at[b_me], (t_flips[mt], k))

    for copy in in_copies:
        copy.wait()

    def send_keys():
        for mt in t_masks:
            unless_me(
                mt,
                middle,
                lambda mt=mt: remote(
                    fk_ref.at[lax.rem(t_flips[mt], heads)],
                    kslot.at[dev_me],
                    k_send,
                    k_recv,
                    (t_flips[mt], middle),
                ),
            )

    pl.when(b_me >= middle)(send_keys)
    k2_copy = pltpu.make_async_copy(sk_hbm.at[head_me], k2buf, k2_sem)
    k2_copy.start()
    block = rows // pieces
    v_copies = [
        pltpu.make_async_copy(
            v_hbm.at[pl.ds(p * block, block)], vbuf.at[pl.ds(p * block, block)], v_sem.at[p]
        )
        for p in range(pieces)
    ]
    for copy in v_copies:
        copy.start()

    for h in range(heads):
        for s in range(seqs):
            icomp[pl.ds(s, 1), pl.ds(h * top, top)] = i_ref[s, pl.ds(h, 1), :]
    islot[slot_me] = icomp[...]
    kslot[dev_me] = fk_ref[head_me]
    for s in range(seqs):
        one = q_ref[s].astype(jnp.float32)
        for h in range(heads):
            qrows[h, pl.ds(s, 1), :] = one[h : h + 1, :]
    for h in range(heads):
        qsend[h] = qrows[h].astype(jnp.bfloat16)
    place_me = (wave_me * heads + head_me) * deep + deep_me
    qslot[place_me] = qsend[head_me]

    for k in (middle, *(k for k in range(nb) if k != middle)):

        @pl.when(b_me < k)
        def _():
            pl.semaphore_wait(ready.at[k], nt)

        if k == middle:
            pl.when(b_me < middle)(send_keys)
            for h in range(heads):

                @pl.when(jnp.logical_not(jnp.logical_and(central, head_me == h)))
                def _():
                    remote(
                        qsend.at[h], qslot.at[place_me], q_send, q_recv, (quad_me * heads + h, k)
                    )

        for mt in t_masks:
            unless_me(
                mt,
                k,
                lambda mt=mt, k=k: remote(
                    icomp, islot.at[slot_me], i_send, i_recv, (t_flips[mt], k)
                ),
            )

    drain(islot.at[pl.ds(0, devices - 1)], i_recv)
    for slot in range(devices):
        istage[pl.ds(slot * seqs, seqs), :] = islot[slot]
    k2_copy.wait()

    @pl.when(central)
    def _():
        places = WAVES * heads * deep
        drain(qslot.at[pl.ds(0, places - 1)], q_recv)
        for n in range(places):
            qstage[pl.ds(n * seqs, seqs), :] = qslot[n].astype(jnp.float32)
        q_all = qstage[...].astype(jnp.bfloat16)
        s2 = lax.dot_general(q_all[:, half:], k2buf[...], NT, preferred_element_type=jnp.float32)
        ids = jnp.concatenate(
            [
                istage[
                    pl.ds(pl.multiple_of(w * wave_rows + j * block_rows + quad_me * span, 8), span),
                    :,
                ]
                for w in range(WAVES)
                for j in range(heads)
            ],
            axis=0,
        )
        sub_count = k2buf.shape[0]
        second = pick_lanes(s2, ids & (sub_count - 1))
        drain(kslot.at[pl.ds(0, devices - 1)], k_recv)
        k1 = kslot[...].astype(jnp.float32)
        k1 = k1.reshape(k1.shape[0] * k1.shape[1], half).astype(jnp.bfloat16)
        s1 = lax.dot_general(q_all[:, :half], k1, NT, preferred_element_type=jnp.float32)
        score = second + pick_lanes(s1, lax.shift_right_arithmetic(ids, log2(sub_count)))
        lane = lax.broadcasted_iota(jnp.int32, ids.shape, 1)
        mine = lax.shift_right_arithmetic(lane, log2(top)) == head_me
        best = jnp.max(jnp.where(mine, score, -jnp.inf), axis=1, keepdims=True)
        raised = jnp.where(mine, jnp.exp(jnp.where(mine, score - best, 0.0)), 0.0)
        weights = raised / jnp.sum(raised, axis=1, keepdims=True)
        weights = weights.astype(jnp.bfloat16).astype(jnp.float32)
        for w in range(WAVES):
            packed = jnp.zeros((span, LANES), jnp.float32)
            for j in range(heads):
                first = (w * heads + j) * span
                packed = packed + pltpu.roll(
                    weights[first : first + span, :],
                    lax.rem(j - head_me + heads, heads) * top,
                    1,
                )
            wpack[pl.ds(w * span, span), :] = packed.astype(jnp.bfloat16)
        where_me = head_me * quads + quad_me
        wslot[where_me] = wpack[...]
        for k in sorted(range(nb), key=lambda k: abs(k - middle), reverse=True):
            for mt in t_masks:
                unless_me(
                    mt,
                    k,
                    lambda mt=mt, k=k: remote(
                        wpack, wslot.at[where_me], w_send, w_recv, (t_flips[mt], k)
                    ),
                )

    high_iota = lax.broadcasted_iota(jnp.int32, (high_count, LANES), 0)
    low_iota = lax.broadcasted_iota(jnp.int32, (LANES, LANES), 0)
    high_hot = high_iota.astype(jnp.float32).astype(jnp.bfloat16)
    low_lane = lax.broadcasted_iota(jnp.int32, (LANES, LANES), 1)
    low_lane = low_lane.astype(jnp.float32).astype(jnp.bfloat16)
    base = dev_me * rows
    one, zero = jnp.bfloat16(1.0), jnp.bfloat16(0.0)

    def build_masks():
        entries = istage[...]
        highrow[...] = lax.shift_right_arithmetic(entries - base, 7).astype(jnp.float32)

        def build(step, carry):
            first = pl.multiple_of(step * GROUP, GROUP)
            some = (istage[pl.ds(first, GROUP), :] & (LANES - 1)).astype(jnp.float32).T
            for u in range(GROUP):
                column = jnp.broadcast_to(some[:, u : u + 1], (LANES, LANES))
                lows[first + u] = jnp.where(low_lane == column.astype(jnp.bfloat16), one, zero)
                row = jnp.broadcast_to(highrow[pl.ds(first + u, 1), :], (high_count, LANES))
                highs[first + u] = jnp.where(high_hot == row.astype(jnp.bfloat16), one, zero)
            return carry

        lax.fori_loop(0, all_seqs // GROUP, build, 0)

    if early:
        build_masks()

    piece = width // chunks
    chip_me = lax.div(t_me, 2) * nb + b_me
    chips = devices // 2
    lane = lax.broadcasted_iota(jnp.int32, (block_rows, LANES), 1)
    block_of = lax.shift_right_arithmetic(lane, log2(top))
    def weigh():
        drain_count(central, lambda n: wslot.at[pl.ds(0, n)], heads * quads, w_recv)
        for w in range(WAVES):
            parts = [
                wslot[pl.ds(h * quads, quads), pl.ds(w * span, span), :]
                .astype(jnp.float32)
                .reshape(block_rows, LANES)
                for h in range(heads)
            ]
            for j in range(heads):
                total = jnp.zeros((block_rows, LANES), jnp.float32)
                for h in range(heads):
                    part = parts[h]
                    if h != j:
                        part = pltpu.roll(part, (h - j) % heads * top, 1)
                    total = jnp.where(block_of == h, part, total)
                wfin[pl.ds(w * wave_rows + j * block_rows, block_rows), :] = total

        def spread(step, carry):
            for u in range(128):
                s = step * 128 + u
                weight = wfin[pl.ds(s, 1), :]
                if early:
                    left = highs[s] * jnp.broadcast_to(weight, (high_count, LANES)).astype(
                        jnp.bfloat16
                    )
                    got = lax.dot_general(left, lows[s], NN, preferred_element_type=jnp.float32)
                else:
                    row = istage[pl.ds(s, 1), :]
                    high = lax.shift_right_arithmetic(row - base, 7)
                    left = jnp.where(high_iota == high, weight, 0.0).astype(jnp.bfloat16)
                    low = jnp.where(low_iota == (row & (LANES - 1)), 1.0, 0.0)
                    got = lax.dot_general(
                        left, low.astype(jnp.bfloat16), NT, preferred_element_type=jnp.float32
                    )
                wacc[pl.ds(s, high_count, stride=pitch), :] = got
            return carry

        lax.fori_loop(0, all_seqs // 128, spread, 0)

        for step in range(high_count):
            wb[:, pl.ds(step * LANES, LANES)] = wacc[pl.ds(step * pitch, all_seqs), :].astype(
                jnp.bfloat16
            )

    def multiply(c):
        acc = jnp.dot(
            wb[...], vbuf[:, pl.ds(c * piece, piece)], preferred_element_type=jnp.float32
        )
        for w in range(WAVES):
            for j in range(heads):
                first = w * wave_rows + j * block_rows
                accs[w, c, j] = acc[first : first + block_rows, :]
        if c == chunks - 1:
            for t in range(2 * DIRECT):
                first = t % heads * block_rows + t // heads * span
                dsend[t] = acc[first : first + seqs, :].astype(jnp.bfloat16)
                mine = jnp.logical_and(t_me == t, b_me == 0)

                @pl.when(jnp.logical_not(mine))
                def _():
                    remote(dsend.at[t], dslot.at[dev_me], d_send, d_recv, (t, 0))

                @pl.when(mine)
                def _():
                    dslot[dev_me] = dsend[t]

        for w in range(WAVES):
            for i in range(heads // 2):
                remote(
                    accs.at[w, c, 2 * i + 1 - core_me],
                    pair.at[w, c, i],
                    a_send.at[w, c],
                    a_recv.at[w, c],
                    (t_me + 1 - 2 * core_me, b_me),
                )

    def pass_on(w, c):
        drain(pair.at[w, c], a_recv.at[w, c])
        per = quads * deep
        for i in range(heads // 2):
            both = accs[w, c, 2 * i + core_me] + pair[w, c, i]
            for g in range(per):
                psend[w, c, i * per + g] = both[g * seqs : (g + 1) * seqs, :].astype(jnp.bfloat16)
        for d in range(deep):
            for chip in range(nt // 2):
                k = w * deep + d
                if c == chunks - 1 and k == 0 and chip < DIRECT:
                    continue
                place = chip % (heads // 2) * per + chip // (heads // 2) * deep + d
                mine = jnp.logical_and(lax.div(t_me, 2) == chip, b_me == k)

                @pl.when(jnp.logical_not(mine))
                def _():
                    remote(
                        psend.at[w, c, place],
                        pslot.at[c, chip_me],
                        p_send.at[c],
                        p_recv.at[c],
                        (2 * chip + core_me, k),
                    )

                @pl.when(mine)
                def _():
                    pslot[c, chip_me] = psend[w, c, place]

    for copy in v_copies:
        copy.wait()
    weigh()
    for c in range(chunks + 1):
        if c < chunks:
            multiply(c)
        if c > 0:
            for w in range(WAVES):
                pass_on(w, c - 1)

    def finish(c, ref, count, sem):
        drain(ref.at[pl.ds(0, count - 1)], sem)
        total = jnp.zeros((seqs, piece), jnp.float32)
        for slot in range(count):
            total = total + ref[slot].astype(jnp.float32)
        out_ref[:, pl.ds(c * piece, piece)] = total.astype(jnp.bfloat16)

    last = chunks - 1
    for c in range(last):
        finish(c, pslot.at[c], chips, p_recv.at[c])
    pl.when(direct)(lambda: finish(last, dslot, devices, d_recv))
    pl.when(jnp.logical_not(direct))(
        lambda: finish(last, pslot.at[last], chips, p_recv.at[last])
    )

    drain_count(central, lambda n: qslot.at[pl.ds(0, n)], heads, q_send)
    drain_count(central, lambda n: kslot.at[pl.ds(0, n)], nt, k_send)
    drain(islot.at[pl.ds(0, devices - 1)], i_send)

    @pl.when(central)
    def _():
        drain(wacc.at[pl.ds(0, (devices - 1) * WAVES * span // 2)], w_send)

    for c in range(chunks):
        if c < last:
            drain(pslot.at[c, pl.ds(0, chips - 1)], p_send.at[c])
        for w in range(WAVES):
            drain(pair.at[w, c], a_send.at[w, c])
    drain_count(
        jnp.logical_not(direct),
        lambda n: pslot.at[last, pl.ds(0, n)],
        chips - DIRECT,
        p_send.at[last],
    )
    drain_count(direct, lambda n: dsend.at[pl.ds(0, n)], 2 * DIRECT, d_send)


def shards(nt, nb, queries, indices, first_keys, second_keys, values):
    seqs, heads, top = indices.shape
    width_q = queries.shape[2]
    half = width_q // 2
    firsts = first_keys.shape[1]
    sub_count = second_keys.shape[1]
    rows, width = values.shape
    devices = nt * nb
    all_seqs = devices * seqs
    deep = nb // WAVES
    quads = nt // heads
    span = deep * seqs
    assert heads * top == LANES and nt % heads == 0 and heads % 2 == 0
    assert nb % WAVES == 0 and span % 8 == 0
    chunks, pieces = 2, 4
    early = all_seqs <= 256
    held = all_seqs if early else 1
    piece = width // chunks
    per_pair = (heads // 2) * quads * deep
    hbm = pl.BlockSpec(memory_space=pltpu.MemorySpace.HBM)
    dma = pltpu.SemaphoreType.DMA
    return pl.pallas_call(
        functools.partial(kernel, (nt, nb, heads, seqs, top, chunks, pieces, early)),
        out_shape=pltpu.VMEM((seqs, width), jnp.bfloat16),
        in_specs=[hbm] * 5,
        out_specs=pl.BlockSpec(memory_space=pltpu.VMEM),
        scratch_shapes=[
            pltpu.VMEM(queries.shape, queries.dtype),
            pltpu.VMEM(indices.shape, indices.dtype),
            pltpu.VMEM(first_keys.shape, first_keys.dtype),
            pltpu.VMEM((rows, width), jnp.bfloat16),
            pltpu.VMEM((sub_count, half), jnp.bfloat16),
            pltpu.VMEM((devices, firsts, half), jnp.bfloat16),
            pltpu.VMEM((devices, seqs, LANES), jnp.int32),
            pltpu.VMEM((seqs, LANES), jnp.int32),
            pltpu.VMEM((heads, seqs, width_q), jnp.float32),
            pltpu.VMEM((heads, seqs, width_q), jnp.bfloat16),
            pltpu.VMEM((heads * nb, seqs, width_q), jnp.bfloat16),
            pltpu.VMEM((heads * nb * seqs, width_q), jnp.float32),
            pltpu.VMEM((WAVES * span, LANES), jnp.bfloat16),
            pltpu.VMEM((heads * quads, WAVES * span, LANES), jnp.bfloat16),
            pltpu.VMEM((all_seqs, LANES), jnp.int32),
            pltpu.VMEM((all_seqs, LANES), jnp.float32),
            pltpu.VMEM((rows // LANES * (all_seqs + 4), LANES), jnp.float32),
            pltpu.VMEM((all_seqs, rows), jnp.bfloat16),
            pltpu.VMEM((held, rows // LANES, LANES), jnp.bfloat16),
            pltpu.VMEM((held, LANES, LANES), jnp.bfloat16),
            pltpu.VMEM((all_seqs, LANES), jnp.float32),
            pltpu.VMEM((WAVES, chunks, heads, quads * span, piece), jnp.float32),
            pltpu.VMEM((WAVES, chunks, heads // 2, quads * span, piece), jnp.float32),
            pltpu.VMEM((WAVES, chunks, per_pair, seqs, piece), jnp.bfloat16),
            pltpu.VMEM((chunks, devices // 2, seqs, piece), jnp.bfloat16),
            pltpu.VMEM((2 * DIRECT, seqs, piece), jnp.bfloat16),
            pltpu.VMEM((devices, seqs, piece), jnp.bfloat16),
            pltpu.SemaphoreType.REGULAR((nb,)),
            dma((3,)),
            dma((pieces,)),
            dma,
            dma,
            dma,
            dma,
            dma,
            dma,
            dma,
            dma,
            dma,
            dma((WAVES, chunks)),
            dma((WAVES, chunks)),
            dma((chunks,)),
            dma((chunks,)),
            dma,
            dma,
        ],
        compiler_params=pltpu.CompilerParams(
            collective_id=0, has_side_effects=True, vmem_limit_bytes=56 * 1024 * 1024
        ),
    )(queries, indices, first_keys, second_keys, values)


def solution(mesh):
    placed = (
        P(("table", "batch"), None, None),
        P(("table", "batch"), None, None),
        P(None, ("table", "batch"), None),
        P(),
        P(("table", "batch"), None),
    )
    body = functools.partial(shards, mesh.shape["table"], mesh.shape["batch"])
    return jax.shard_map(
        body, mesh=mesh, in_specs=placed, out_specs=P(("table", "batch"), None), check_vma=False
    )
```

```python
import functools

import jax
import jax.numpy as jnp
from jax import lax
from jax.experimental import pallas as pl
from jax.experimental.pallas import tpu as pltpu
from jax.sharding import PartitionSpec as P

MESH = pl.DeviceIdType.MESH
LANES = 128
NT = (((1,), (1,)), ((), ()))
NN = (((1,), (0,)), ((), ()))
WAVES = 2
GROUP = 32
DIRECT = 1


def log2(number):
    assert number & (number - 1) == 0
    return number.bit_length() - 1


def pick_lanes(table, ids):
    picked = jnp.zeros(ids.shape, jnp.float32)
    inner = ids & (LANES - 1)
    outer = lax.shift_right_arithmetic(ids, 7)
    for part in range(table.shape[1] // LANES):
        got = jnp.take_along_axis(table[:, part * LANES : (part + 1) * LANES], inner, axis=1)
        picked = jnp.where(outer == part, got, picked)
    return picked


def kernel(
    shape,
    q_hbm,
    i_hbm,
    fk_hbm,
    sk_hbm,
    v_hbm,
    out_ref,
    q_ref,
    i_ref,
    fk_ref,
    vbuf,
    k2buf,
    kslot,
    islot,
    icomp,
    qrows,
    qsend,
    qslot,
    qstage,
    cids,
    wpack,
    wslot,
    istage,
    wfin,
    wacc,
    wb,
    highs,
    lows,
    highrow,
    accs,
    pair,
    psend,
    pslot,
    dsend,
    dslot,
    ready,
    in_sem,
    v_sem,
    k2_sem,
    k_send,
    k_recv,
    i_send,
    i_recv,
    q_send,
    q_recv,
    w_send,
    w_recv,
    a_send,
    a_recv,
    p_send,
    p_recv,
    d_send,
    d_recv,
):
    nt, nb, heads, seqs, top, chunks, pieces, early = shape
    devices = nt * nb
    quads = nt // heads
    deep = nb // WAVES
    middle = deep - 1
    span = deep * seqs
    block_rows = quads * span
    wave_rows = heads * block_rows
    wave_devs = nt * deep
    all_seqs = devices * seqs
    half = fk_hbm.shape[2]
    rows, width = v_hbm.shape
    high_count = rows // LANES
    pitch = all_seqs + 4
    t_me, b_me = lax.axis_index("table"), lax.axis_index("batch")
    dev_me = t_me * nb + b_me
    core_me = lax.rem(t_me, 2)
    head_me = lax.rem(t_me, heads)
    quad_me = lax.div(t_me, heads)
    wave_me = lax.div(b_me, deep)
    deep_me = lax.rem(b_me, deep)
    central = b_me == middle
    direct = jnp.logical_and(t_me < 2 * DIRECT, b_me == 0)

    def slot_of(t, b):
        return (
            lax.div(b, deep) * wave_devs
            + (lax.rem(t, heads) * quads + lax.div(t, heads)) * deep
            + lax.rem(b, deep)
        )

    def flips(x, count):
        bits = [(x // 2**i) % 2 for i in range(log2(count))]
        return [
            x + sum((1 - 2 * bit) * 2**i for i, bit in enumerate(bits) if mask >> i & 1)
            for mask in range(count)
        ]

    slot_me = slot_of(t_me, b_me)
    t_flips = flips(t_me, nt)
    t_masks = sorted(range(nt), key=lambda m: (bin(m >> 1).count("1"), m), reverse=True)

    def unless_me(mt, k, body):
        if mt:
            body()
        else:
            pl.when(b_me != k)(body)

    def drain(ref, sem):
        pltpu.make_async_copy(ref, ref, sem).wait()

    def drain_count(less, ref_of, count, sem):
        pl.when(less)(lambda: drain(ref_of(count - 1), sem))
        pl.when(jnp.logical_not(less))(lambda: drain(ref_of(count), sem))

    def remote(src, dst, send, recv, where):
        pltpu.make_async_remote_copy(
            src_ref=src,
            dst_ref=dst,
            send_sem=send,
            recv_sem=recv,
            device_id=where,
            device_id_type=MESH,
        ).start()

    in_copies = [
        pltpu.make_async_copy(src, dst, in_sem.at[n])
        for n, (src, dst) in enumerate(((fk_hbm, fk_ref), (i_hbm, i_ref), (q_hbm, q_ref)))
    ]
    for copy in in_copies:
        copy.start()
    barrier = pltpu.get_barrier_semaphore()

    def greet(sem, where):
        pl.semaphore_signal(sem, inc=1, device_id=where, device_id_type=MESH)

    for k in range(nb - 1, -1, -1):

        @pl.when(b_me <= k)
        def _():
            for mt in t_masks:
                unless_me(mt, k, lambda mt=mt: greet(barrier, (t_flips[mt], k)))

    pl.semaphore_wait(barrier, nt * (b_me + 1) - 1)
    for k in range(nb - 1):

        @pl.when(b_me > k)
        def _():
            for mt in t_masks:
                greet(ready.at[b_me], (t_flips[mt], k))

    for copy in in_copies:
        copy.wait()

    def send_keys():
        for mt in t_masks:
            unless_me(
                mt,
                middle,
                lambda mt=mt: remote(
                    fk_ref.at[lax.rem(t_flips[mt], heads)],
                    kslot.at[dev_me],
                    k_send,
                    k_recv,
                    (t_flips[mt], middle),
                ),
            )

    pl.when(b_me >= middle)(send_keys)
    k2_copy = pltpu.make_async_copy(sk_hbm.at[head_me], k2buf, k2_sem)
    k2_copy.start()
    block = rows // pieces
    v_copies = [
        pltpu.make_async_copy(
            v_hbm.at[pl.ds(p * block, block)], vbuf.at[pl.ds(p * block, block)], v_sem.at[p]
        )
        for p in range(pieces)
    ]
    for copy in v_copies:
        copy.start()

    for h in range(heads):
        for s in range(seqs):
            icomp[pl.ds(s, 1), pl.ds(h * top, top)] = i_ref[s, pl.ds(h, 1), :]
    islot[slot_me] = icomp[...]
    kslot[dev_me] = fk_ref[head_me]
    for s in range(seqs):
        one = q_ref[s].astype(jnp.float32)
        for h in range(heads):
            qrows[h, pl.ds(s, 1), :] = one[h : h + 1, :]
    for h in range(heads):
        qsend[h] = qrows[h].astype(jnp.bfloat16)
    place_me = (wave_me * heads + head_me) * deep + deep_me
    qslot[place_me] = qsend[head_me]

    for k in (middle, *(k for k in range(nb) if k != middle)):

        @pl.when(b_me < k)
        def _():
            pl.semaphore_wait(ready.at[k], nt)

        if k == middle:
            pl.when(b_me < middle)(send_keys)
            for h in range(heads):

                @pl.when(jnp.logical_not(jnp.logical_and(central, head_me == h)))
                def _():
                    where = (quad_me * heads + h, k)
                    remote(qsend.at[h], qslot.at[place_me], q_send, q_recv, where)
                    remote(icomp, islot.at[slot_me], i_send, i_recv.at[0], where)

        for mt in t_masks:
            if k != middle or mt >= heads:
                unless_me(
                    mt,
                    k,
                    lambda mt=mt, k=k: remote(
                        icomp, islot.at[slot_me], i_send, i_recv.at[1], (t_flips[mt], k)
                    ),
                )

    k2_copy.wait()

    @pl.when(central)
    def _():
        places = WAVES * heads * deep
        drain(islot.at[pl.ds(0, places - 1)], i_recv.at[0])
        drain(qslot.at[pl.ds(0, places - 1)], q_recv)
        for n in range(places):
            qstage[pl.ds(n * seqs, seqs), :] = qslot[n].astype(jnp.float32)
            row, z = n // deep, n % deep
            from_slot = row // heads * wave_devs + (row % heads * quads + quad_me) * deep + z
            cids[pl.ds(n * seqs, seqs), :] = islot[from_slot]
        q_all = qstage[...].astype(jnp.bfloat16)
        s2 = lax.dot_general(q_all[:, half:], k2buf[...], NT, preferred_element_type=jnp.float32)
        ids = cids[...]
        sub_count = k2buf.shape[0]
        second = pick_lanes(s2, ids & (sub_count - 1))
        drain(kslot.at[pl.ds(0, devices - 1)], k_recv)
        k1 = kslot[...].astype(jnp.float32)
        k1 = k1.reshape(k1.shape[0] * k1.shape[1], half).astype(jnp.bfloat16)
        s1 = lax.dot_general(q_all[:, :half], k1, NT, preferred_element_type=jnp.float32)
        score = second + pick_lanes(s1, lax.shift_right_arithmetic(ids, log2(sub_count)))
        lane = lax.broadcasted_iota(jnp.int32, ids.shape, 1)
        mine = lax.shift_right_arithmetic(lane, log2(top)) == head_me
        best = jnp.max(jnp.where(mine, score, -jnp.inf), axis=1, keepdims=True)
        raised = jnp.where(mine, jnp.exp(jnp.where(mine, score - best, 0.0)), 0.0)
        weights = raised / jnp.sum(raised, axis=1, keepdims=True)
        weights = weights.astype(jnp.bfloat16).astype(jnp.float32)
        for w in range(WAVES):
            packed = jnp.zeros((span, LANES), jnp.float32)
            for j in range(heads):
                first = (w * heads + j) * span
                packed = packed + pltpu.roll(
                    weights[first : first + span, :],
                    lax.rem(j - head_me + heads, heads) * top,
                    1,
                )
            wpack[pl.ds(w * span, span), :] = packed.astype(jnp.bfloat16)
        where_me = head_me * quads + quad_me
        wslot[where_me] = wpack[...]
        for k in sorted(range(nb), key=lambda k: abs(k - middle), reverse=True):
            for mt in t_masks:
                unless_me(
                    mt,
                    k,
                    lambda mt=mt, k=k: remote(
                        wpack, wslot.at[where_me], w_send, w_recv, (t_flips[mt], k)
                    ),
                )

    quad_devs = heads * nb
    pl.when(central)(lambda: drain(islot.at[pl.ds(0, devices - quad_devs)], i_recv.at[1]))
    pl.when(jnp.logical_not(central))(
        lambda: drain(islot.at[pl.ds(0, devices - 1)], i_recv.at[1])
    )
    for slot in range(devices):
        istage[pl.ds(slot * seqs, seqs), :] = islot[slot]
    high_iota = lax.broadcasted_iota(jnp.int32, (high_count, LANES), 0)
    low_iota = lax.broadcasted_iota(jnp.int32, (LANES, LANES), 0)
    high_hot = high_iota.astype(jnp.float32).astype(jnp.bfloat16)
    low_lane = lax.broadcasted_iota(jnp.int32, (LANES, LANES), 1)
    low_lane = low_lane.astype(jnp.float32).astype(jnp.bfloat16)
    base = dev_me * rows
    one, zero = jnp.bfloat16(1.0), jnp.bfloat16(0.0)

    def build_masks():
        entries = istage[...]
        highrow[...] = lax.shift_right_arithmetic(entries - base, 7).astype(jnp.float32)

        def build(step, carry):
            first = pl.multiple_of(step * GROUP, GROUP)
            some = (istage[pl.ds(first, GROUP), :] & (LANES - 1)).astype(jnp.float32).T
            for u in range(GROUP):
                column = jnp.broadcast_to(some[:, u : u + 1], (LANES, LANES))
                lows[first + u] = jnp.where(low_lane == column.astype(jnp.bfloat16), one, zero)
                row = jnp.broadcast_to(highrow[pl.ds(first + u, 1), :], (high_count, LANES))
                highs[first + u] = jnp.where(high_hot == row.astype(jnp.bfloat16), one, zero)
            return carry

        lax.fori_loop(0, all_seqs // GROUP, build, 0)

    if early:
        build_masks()

    piece = width // chunks
    chip_me = lax.div(t_me, 2) * nb + b_me
    chips = devices // 2
    lane = lax.broadcasted_iota(jnp.int32, (block_rows, LANES), 1)
    block_of = lax.shift_right_arithmetic(lane, log2(top))
    def weigh():
        drain_count(central, lambda n: wslot.at[pl.ds(0, n)], heads * quads, w_recv)
        for w in range(WAVES):
            parts = [
                wslot[pl.ds(h * quads, quads), pl.ds(w * span, span), :]
                .astype(jnp.float32)
                .reshape(block_rows, LANES)
                for h in range(heads)
            ]
            for j in range(heads):
                total = jnp.zeros((block_rows, LANES), jnp.float32)
                for h in range(heads):
                    part = parts[h]
                    if h != j:
                        part = pltpu.roll(part, (h - j) % heads * top, 1)
                    total = jnp.where(block_of == h, part, total)
                wfin[pl.ds(w * wave_rows + j * block_rows, block_rows), :] = total

        def spread(step, carry):
            for u in range(128):
                s = step * 128 + u
                weight = wfin[pl.ds(s, 1), :]
                if early:
                    left = highs[s] * jnp.broadcast_to(weight, (high_count, LANES)).astype(
                        jnp.bfloat16
                    )
                    got = lax.dot_general(left, lows[s], NN, preferred_element_type=jnp.float32)
                else:
                    row = istage[pl.ds(s, 1), :]
                    high = lax.shift_right_arithmetic(row - base, 7)
                    left = jnp.where(high_iota == high, weight, 0.0).astype(jnp.bfloat16)
                    low = jnp.where(low_iota == (row & (LANES - 1)), 1.0, 0.0)
                    got = lax.dot_general(
                        left, low.astype(jnp.bfloat16), NT, preferred_element_type=jnp.float32
                    )
                wacc[pl.ds(s, high_count, stride=pitch), :] = got
            return carry

        lax.fori_loop(0, all_seqs // 128, spread, 0)

        for step in range(high_count):
            wb[:, pl.ds(step * LANES, LANES)] = wacc[pl.ds(step * pitch, all_seqs), :].astype(
                jnp.bfloat16
            )

    def multiply(c):
        acc = jnp.dot(
            wb[...], vbuf[:, pl.ds(c * piece, piece)], preferred_element_type=jnp.float32
        )
        for w in range(WAVES):
            for j in range(heads):
                first = w * wave_rows + j * block_rows
                accs[w, c, j] = acc[first : first + block_rows, :]
        if c == chunks - 1:
            for t in range(2 * DIRECT):
                first = t % heads * block_rows + t // heads * span
                dsend[t] = acc[first : first + seqs, :].astype(jnp.bfloat16)
                mine = jnp.logical_and(t_me == t, b_me == 0)

                @pl.when(jnp.logical_not(mine))
                def _():
                    remote(dsend.at[t], dslot.at[dev_me], d_send, d_recv, (t, 0))

                @pl.when(mine)
                def _():
                    dslot[dev_me] = dsend[t]

        for w in range(WAVES):
            for i in range(heads // 2):
                remote(
                    accs.at[w, c, 2 * i + 1 - core_me],
                    pair.at[w, c, i],
                    a_send.at[w, c],
                    a_recv.at[w, c],
                    (t_me + 1 - 2 * core_me, b_me),
                )

    def pass_on(w, c):
        drain(pair.at[w, c], a_recv.at[w, c])
        per = quads * deep
        for i in range(heads // 2):
            both = accs[w, c, 2 * i + core_me] + pair[w, c, i]
            for g in range(per):
                psend[w, c, i * per + g] = both[g * seqs : (g + 1) * seqs, :].astype(jnp.bfloat16)
        for d in range(deep):
            for chip in range(nt // 2):
                k = w * deep + d
                if c == chunks - 1 and k == 0 and chip < DIRECT:
                    continue
                place = chip % (heads // 2) * per + chip // (heads // 2) * deep + d
                mine = jnp.logical_and(lax.div(t_me, 2) == chip, b_me == k)

                @pl.when(jnp.logical_not(mine))
                def _():
                    remote(
                        psend.at[w, c, place],
                        pslot.at[c, chip_me],
                        p_send.at[c],
                        p_recv.at[c],
                        (2 * chip + core_me, k),
                    )

                @pl.when(mine)
                def _():
                    pslot[c, chip_me] = psend[w, c, place]

    for copy in v_copies:
        copy.wait()
    weigh()
    for c in range(chunks + 1):
        if c < chunks:
            multiply(c)
        if c > 0:
            for w in range(WAVES):
                pass_on(w, c - 1)

    def finish(c, ref, count, sem):
        drain(ref.at[pl.ds(0, count - 1)], sem)
        total = jnp.zeros((seqs, piece), jnp.float32)
        for slot in range(count):
            total = total + ref[slot].astype(jnp.float32)
        out_ref[:, pl.ds(c * piece, piece)] = total.astype(jnp.bfloat16)

    last = chunks - 1
    for c in range(last):
        finish(c, pslot.at[c], chips, p_recv.at[c])
    pl.when(direct)(lambda: finish(last, dslot, devices, d_recv))
    pl.when(jnp.logical_not(direct))(
        lambda: finish(last, pslot.at[last], chips, p_recv.at[last])
    )

    drain_count(central, lambda n: qslot.at[pl.ds(0, n)], heads, q_send)
    drain_count(central, lambda n: kslot.at[pl.ds(0, n)], nt, k_send)
    drain(islot.at[pl.ds(0, devices - 1)], i_send)

    @pl.when(central)
    def _():
        drain(wacc.at[pl.ds(0, (devices - 1) * WAVES * span // 2)], w_send)

    for c in range(chunks):
        if c < last:
            drain(pslot.at[c, pl.ds(0, chips - 1)], p_send.at[c])
        for w in range(WAVES):
            drain(pair.at[w, c], a_send.at[w, c])
    drain_count(
        jnp.logical_not(direct),
        lambda n: pslot.at[last, pl.ds(0, n)],
        chips - DIRECT,
        p_send.at[last],
    )
    drain_count(direct, lambda n: dsend.at[pl.ds(0, n)], 2 * DIRECT, d_send)


def shards(nt, nb, queries, indices, first_keys, second_keys, values):
    seqs, heads, top = indices.shape
    width_q = queries.shape[2]
    half = width_q // 2
    firsts = first_keys.shape[1]
    sub_count = second_keys.shape[1]
    rows, width = values.shape
    devices = nt * nb
    all_seqs = devices * seqs
    deep = nb // WAVES
    quads = nt // heads
    span = deep * seqs
    assert heads * top == LANES and nt % heads == 0 and heads % 2 == 0
    assert nb % WAVES == 0 and span % 8 == 0
    chunks, pieces = 2, 4
    early = all_seqs <= 256
    held = all_seqs if early else 1
    piece = width // chunks
    per_pair = (heads // 2) * quads * deep
    hbm = pl.BlockSpec(memory_space=pltpu.MemorySpace.HBM)
    dma = pltpu.SemaphoreType.DMA
    return pl.pallas_call(
        functools.partial(kernel, (nt, nb, heads, seqs, top, chunks, pieces, early)),
        out_shape=pltpu.VMEM((seqs, width), jnp.bfloat16),
        in_specs=[hbm] * 5,
        out_specs=pl.BlockSpec(memory_space=pltpu.VMEM),
        scratch_shapes=[
            pltpu.VMEM(queries.shape, queries.dtype),
            pltpu.VMEM(indices.shape, indices.dtype),
            pltpu.VMEM(first_keys.shape, first_keys.dtype),
            pltpu.VMEM((rows, width), jnp.bfloat16),
            pltpu.VMEM((sub_count, half), jnp.bfloat16),
            pltpu.VMEM((devices, firsts, half), jnp.bfloat16),
            pltpu.VMEM((devices, seqs, LANES), jnp.int32),
            pltpu.VMEM((seqs, LANES), jnp.int32),
            pltpu.VMEM((heads, seqs, width_q), jnp.float32),
            pltpu.VMEM((heads, seqs, width_q), jnp.bfloat16),
            pltpu.VMEM((heads * nb, seqs, width_q), jnp.bfloat16),
            pltpu.VMEM((heads * nb * seqs, width_q), jnp.float32),
            pltpu.VMEM((heads * nb * seqs, LANES), jnp.int32),
            pltpu.VMEM((WAVES * span, LANES), jnp.bfloat16),
            pltpu.VMEM((heads * quads, WAVES * span, LANES), jnp.bfloat16),
            pltpu.VMEM((all_seqs, LANES), jnp.int32),
            pltpu.VMEM((all_seqs, LANES), jnp.float32),
            pltpu.VMEM((rows // LANES * (all_seqs + 4), LANES), jnp.float32),
            pltpu.VMEM((all_seqs, rows), jnp.bfloat16),
            pltpu.VMEM((held, rows // LANES, LANES), jnp.bfloat16),
            pltpu.VMEM((held, LANES, LANES), jnp.bfloat16),
            pltpu.VMEM((all_seqs, LANES), jnp.float32),
            pltpu.VMEM((WAVES, chunks, heads, quads * span, piece), jnp.float32),
            pltpu.VMEM((WAVES, chunks, heads // 2, quads * span, piece), jnp.float32),
            pltpu.VMEM((WAVES, chunks, per_pair, seqs, piece), jnp.bfloat16),
            pltpu.VMEM((chunks, devices // 2, seqs, piece), jnp.bfloat16),
            pltpu.VMEM((2 * DIRECT, seqs, piece), jnp.bfloat16),
            pltpu.VMEM((devices, seqs, piece), jnp.bfloat16),
            pltpu.SemaphoreType.REGULAR((nb,)),
            dma((3,)),
            dma((pieces,)),
            dma,
            dma,
            dma,
            dma,
            dma((2,)),
            dma,
            dma,
            dma,
            dma,
            dma((WAVES, chunks)),
            dma((WAVES, chunks)),
            dma((chunks,)),
            dma((chunks,)),
            dma,
            dma,
        ],
        compiler_params=pltpu.CompilerParams(
            collective_id=0, has_side_effects=True, vmem_limit_bytes=56 * 1024 * 1024
        ),
    )(queries, indices, first_keys, second_keys, values)


def solution(mesh):
    placed = (
        P(("table", "batch"), None, None),
        P(("table", "batch"), None, None),
        P(None, ("table", "batch"), None),
        P(),
        P(("table", "batch"), None),
    )
    body = functools.partial(shards, mesh.shape["table"], mesh.shape["batch"])
    return jax.shard_map(
        body, mesh=mesh, in_specs=placed, out_specs=P(("table", "batch"), None), check_vma=False
    )
```

```python
import functools

import jax
import jax.numpy as jnp
from jax import lax
from jax.experimental import pallas as pl
from jax.experimental.pallas import tpu as pltpu
from jax.sharding import PartitionSpec as P

MESH = pl.DeviceIdType.MESH
LANES = 128
NT = (((1,), (1,)), ((), ()))
NN = (((1,), (0,)), ((), ()))
WAVES = 2
GROUP = 32
DIRECT = 1


def log2(number):
    assert number & (number - 1) == 0
    return number.bit_length() - 1


def pick_lanes(table, ids):
    picked = jnp.zeros(ids.shape, jnp.float32)
    inner = ids & (LANES - 1)
    outer = lax.shift_right_arithmetic(ids, 7)
    for part in range(table.shape[1] // LANES):
        got = jnp.take_along_axis(table[:, part * LANES : (part + 1) * LANES], inner, axis=1)
        picked = jnp.where(outer == part, got, picked)
    return picked


def kernel(
    shape,
    q_hbm,
    i_hbm,
    fk_hbm,
    sk_hbm,
    v_hbm,
    out_ref,
    q_ref,
    i_ref,
    fk_ref,
    vbuf,
    k2buf,
    kslot,
    islot,
    icomp,
    qrows,
    qsend,
    qslot,
    qstage,
    cids,
    wpack,
    wslot,
    istage,
    wfin,
    wacc,
    wb,
    highs,
    lows,
    highrow,
    accs,
    pair,
    psend,
    pslot,
    dsend,
    dslot,
    ready,
    in_sem,
    v_sem,
    k2_sem,
    k_send,
    k_recv,
    i_send,
    i_recv,
    q_send,
    q_recv,
    w_send,
    w_recv,
    a_send,
    a_recv,
    p_send,
    p_recv,
    d_send,
    d_recv,
):
    nt, nb, heads, seqs, top, chunks, pieces, early = shape
    devices = nt * nb
    quads = nt // heads
    deep = nb // WAVES
    middle = deep - 1
    span = deep * seqs
    block_rows = quads * span
    wave_rows = heads * block_rows
    wave_devs = nt * deep
    all_seqs = devices * seqs
    half = fk_hbm.shape[2]
    rows, width = v_hbm.shape
    high_count = rows // LANES
    pitch = all_seqs + 4
    t_me, b_me = lax.axis_index("table"), lax.axis_index("batch")
    dev_me = t_me * nb + b_me
    core_me = lax.rem(t_me, 2)
    head_me = lax.rem(t_me, heads)
    quad_me = lax.div(t_me, heads)
    wave_me = lax.div(b_me, deep)
    deep_me = lax.rem(b_me, deep)
    central = b_me == middle
    direct = jnp.logical_and(t_me < 2 * DIRECT, b_me == 0)

    def slot_of(t, b):
        return (
            lax.div(b, deep) * wave_devs
            + (lax.rem(t, heads) * quads + lax.div(t, heads)) * deep
            + lax.rem(b, deep)
        )

    def flips(x, count):
        bits = [(x // 2**i) % 2 for i in range(log2(count))]
        return [
            x + sum((1 - 2 * bit) * 2**i for i, bit in enumerate(bits) if mask >> i & 1)
            for mask in range(count)
        ]

    slot_me = slot_of(t_me, b_me)
    t_flips = flips(t_me, nt)
    t_masks = sorted(range(nt), key=lambda m: (bin(m >> 1).count("1"), m), reverse=True)

    def unless_me(mt, k, body):
        if mt:
            body()
        else:
            pl.when(b_me != k)(body)

    def drain(ref, sem):
        pltpu.make_async_copy(ref, ref, sem).wait()

    def drain_count(less, ref_of, count, sem):
        pl.when(less)(lambda: drain(ref_of(count - 1), sem))
        pl.when(jnp.logical_not(less))(lambda: drain(ref_of(count), sem))

    def remote(src, dst, send, recv, where):
        pltpu.make_async_remote_copy(
            src_ref=src,
            dst_ref=dst,
            send_sem=send,
            recv_sem=recv,
            device_id=where,
            device_id_type=MESH,
        ).start()

    in_copies = [
        pltpu.make_async_copy(src, dst, in_sem.at[n])
        for n, (src, dst) in enumerate(((fk_hbm, fk_ref), (i_hbm, i_ref), (q_hbm, q_ref)))
    ]
    for copy in in_copies:
        copy.start()
    barrier = pltpu.get_barrier_semaphore()

    def greet(sem, where):
        pl.semaphore_signal(sem, inc=1, device_id=where, device_id_type=MESH)

    for k in range(nb - 1, -1, -1):

        @pl.when(b_me <= k)
        def _():
            for mt in t_masks:
                unless_me(mt, k, lambda mt=mt: greet(barrier, (t_flips[mt], k)))

    pl.semaphore_wait(barrier, nt * (b_me + 1) - 1)
    for k in range(nb - 1):

        @pl.when(b_me > k)
        def _():
            for mt in t_masks:
                greet(ready.at[b_me], (t_flips[mt], k))

    for copy in in_copies:
        copy.wait()

    def send_keys():
        for mt in t_masks:
            unless_me(
                mt,
                middle,
                lambda mt=mt: remote(
                    fk_ref.at[lax.rem(t_flips[mt], heads)],
                    kslot.at[dev_me],
                    k_send,
                    k_recv,
                    (t_flips[mt], middle),
                ),
            )

    pl.when(b_me >= middle)(send_keys)
    k2_copy = pltpu.make_async_copy(sk_hbm.at[head_me], k2buf, k2_sem)
    k2_copy.start()
    for h in range(heads):
        for s in range(seqs):
            icomp[pl.ds(s, 1), pl.ds(h * top, top)] = i_ref[s, pl.ds(h, 1), :]
    islot[slot_me] = icomp[...]
    kslot[dev_me] = fk_ref[head_me]
    for s in range(seqs):
        one = q_ref[s].astype(jnp.float32)
        for h in range(heads):
            qrows[h, pl.ds(s, 1), :] = one[h : h + 1, :]
    for h in range(heads):
        qsend[h] = qrows[h].astype(jnp.bfloat16)
    place_me = (wave_me * heads + head_me) * deep + deep_me
    qslot[place_me] = qsend[head_me]

    for k in (middle, *(k for k in range(nb) if k != middle)):

        @pl.when(b_me < k)
        def _():
            pl.semaphore_wait(ready.at[k], nt)

        if k == middle:
            pl.when(b_me < middle)(send_keys)
            for h in range(heads):

                @pl.when(jnp.logical_not(jnp.logical_and(central, head_me == h)))
                def _():
                    where = (quad_me * heads + h, k)
                    remote(qsend.at[h], qslot.at[place_me], q_send, q_recv, where)
                    remote(icomp, islot.at[slot_me], i_send, i_recv.at[0], where)

        for mt in t_masks:
            if k != middle or mt >= heads:
                unless_me(
                    mt,
                    k,
                    lambda mt=mt, k=k: remote(
                        icomp, islot.at[slot_me], i_send, i_recv.at[1], (t_flips[mt], k)
                    ),
                )

    block = rows // pieces
    v_copies = [
        pltpu.make_async_copy(
            v_hbm.at[pl.ds(p * block, block)], vbuf.at[pl.ds(p * block, block)], v_sem.at[p]
        )
        for p in range(pieces)
    ]
    for copy in v_copies:
        copy.start()

    k2_copy.wait()

    @pl.when(central)
    def _():
        places = WAVES * heads * deep
        drain(islot.at[pl.ds(0, places - 1)], i_recv.at[0])
        drain(qslot.at[pl.ds(0, places - 1)], q_recv)
        for n in range(places):
            qstage[pl.ds(n * seqs, seqs), :] = qslot[n].astype(jnp.float32)
            row, z = n // deep, n % deep
            from_slot = row // heads * wave_devs + (row % heads * quads + quad_me) * deep + z
            cids[pl.ds(n * seqs, seqs), :] = islot[from_slot]
        q_all = qstage[...].astype(jnp.bfloat16)
        s2 = lax.dot_general(q_all[:, half:], k2buf[...], NT, preferred_element_type=jnp.float32)
        ids = cids[...]
        sub_count = k2buf.shape[0]
        second = pick_lanes(s2, ids & (sub_count - 1))
        drain(kslot.at[pl.ds(0, devices - 1)], k_recv)
        k1 = kslot[...].astype(jnp.float32)
        k1 = k1.reshape(k1.shape[0] * k1.shape[1], half).astype(jnp.bfloat16)
        s1 = lax.dot_general(q_all[:, :half], k1, NT, preferred_element_type=jnp.float32)
        score = second + pick_lanes(s1, lax.shift_right_arithmetic(ids, log2(sub_count)))
        lane = lax.broadcasted_iota(jnp.int32, ids.shape, 1)
        mine = lax.shift_right_arithmetic(lane, log2(top)) == head_me
        best = jnp.max(jnp.where(mine, score, -jnp.inf), axis=1, keepdims=True)
        raised = jnp.where(mine, jnp.exp(jnp.where(mine, score - best, 0.0)), 0.0)
        weights = raised / jnp.sum(raised, axis=1, keepdims=True)
        weights = weights.astype(jnp.bfloat16).astype(jnp.float32)
        for w in range(WAVES):
            packed = jnp.zeros((span, LANES), jnp.float32)
            for j in range(heads):
                first = (w * heads + j) * span
                packed = packed + pltpu.roll(
                    weights[first : first + span, :],
                    lax.rem(j - head_me + heads, heads) * top,
                    1,
                )
            wpack[pl.ds(w * span, span), :] = packed.astype(jnp.bfloat16)
        where_me = head_me * quads + quad_me
        wslot[where_me] = wpack[...]
        for k in sorted(range(nb), key=lambda k: abs(k - middle), reverse=True):
            for mt in t_masks:
                unless_me(
                    mt,
                    k,
                    lambda mt=mt, k=k: remote(
                        wpack, wslot.at[where_me], w_send, w_recv, (t_flips[mt], k)
                    ),
                )

    quad_devs = heads * nb
    pl.when(central)(lambda: drain(islot.at[pl.ds(0, devices - quad_devs)], i_recv.at[1]))
    pl.when(jnp.logical_not(central))(
        lambda: drain(islot.at[pl.ds(0, devices - 1)], i_recv.at[1])
    )
    for slot in range(devices):
        istage[pl.ds(slot * seqs, seqs), :] = islot[slot]
    high_iota = lax.broadcasted_iota(jnp.int32, (high_count, LANES), 0)
    low_iota = lax.broadcasted_iota(jnp.int32, (LANES, LANES), 0)
    high_hot = high_iota.astype(jnp.float32).astype(jnp.bfloat16)
    low_lane = lax.broadcasted_iota(jnp.int32, (LANES, LANES), 1)
    low_lane = low_lane.astype(jnp.float32).astype(jnp.bfloat16)
    base = dev_me * rows
    one, zero = jnp.bfloat16(1.0), jnp.bfloat16(0.0)

    def build_masks():
        entries = istage[...]
        highrow[...] = lax.shift_right_arithmetic(entries - base, 7).astype(jnp.float32)

        def build(step, carry):
            first = pl.multiple_of(step * GROUP, GROUP)
            some = (istage[pl.ds(first, GROUP), :] & (LANES - 1)).astype(jnp.float32).T
            for u in range(GROUP):
                column = jnp.broadcast_to(some[:, u : u + 1], (LANES, LANES))
                lows[first + u] = jnp.where(low_lane == column.astype(jnp.bfloat16), one, zero)
                row = jnp.broadcast_to(highrow[pl.ds(first + u, 1), :], (high_count, LANES))
                highs[first + u] = jnp.where(high_hot == row.astype(jnp.bfloat16), one, zero)
            return carry

        lax.fori_loop(0, all_seqs // GROUP, build, 0)

    if early:
        build_masks()

    piece = width // chunks
    chip_me = lax.div(t_me, 2) * nb + b_me
    chips = devices // 2
    lane = lax.broadcasted_iota(jnp.int32, (block_rows, LANES), 1)
    block_of = lax.shift_right_arithmetic(lane, log2(top))
    def weigh():
        drain_count(central, lambda n: wslot.at[pl.ds(0, n)], heads * quads, w_recv)
        for w in range(WAVES):
            parts = [
                wslot[pl.ds(h * quads, quads), pl.ds(w * span, span), :]
                .astype(jnp.float32)
                .reshape(block_rows, LANES)
                for h in range(heads)
            ]
            for j in range(heads):
                total = jnp.zeros((block_rows, LANES), jnp.float32)
                for h in range(heads):
                    part = parts[h]
                    if h != j:
                        part = pltpu.roll(part, (h - j) % heads * top, 1)
                    total = jnp.where(block_of == h, part, total)
                wfin[pl.ds(w * wave_rows + j * block_rows, block_rows), :] = total

        def spread(step, carry):
            for u in range(128):
                s = step * 128 + u
                weight = wfin[pl.ds(s, 1), :]
                if early:
                    left = highs[s] * jnp.broadcast_to(weight, (high_count, LANES)).astype(
                        jnp.bfloat16
                    )
                    got = lax.dot_general(left, lows[s], NN, preferred_element_type=jnp.float32)
                else:
                    row = istage[pl.ds(s, 1), :]
                    high = lax.shift_right_arithmetic(row - base, 7)
                    left = jnp.where(high_iota == high, weight, 0.0).astype(jnp.bfloat16)
                    low = jnp.where(low_iota == (row & (LANES - 1)), 1.0, 0.0)
                    got = lax.dot_general(
                        left, low.astype(jnp.bfloat16), NT, preferred_element_type=jnp.float32
                    )
                wacc[pl.ds(s, high_count, stride=pitch), :] = got
            return carry

        lax.fori_loop(0, all_seqs // 128, spread, 0)

        for step in range(high_count):
            wb[:, pl.ds(step * LANES, LANES)] = wacc[pl.ds(step * pitch, all_seqs), :].astype(
                jnp.bfloat16
            )

    def multiply(c):
        acc = jnp.dot(
            wb[...], vbuf[:, pl.ds(c * piece, piece)], preferred_element_type=jnp.float32
        )
        for w in range(WAVES):
            for j in range(heads):
                first = w * wave_rows + j * block_rows
                accs[w, c, j] = acc[first : first + block_rows, :]
        for t in range(2 * DIRECT):
            first = t % heads * block_rows + t // heads * span
            dsend[c, t] = acc[first : first + seqs, :].astype(jnp.bfloat16)
            mine = jnp.logical_and(t_me == t, b_me == 0)

            @pl.when(jnp.logical_not(mine))
            def _():
                remote(dsend.at[c, t], dslot.at[c, dev_me], d_send.at[c], d_recv.at[c], (t, 0))

            @pl.when(mine)
            def _():
                dslot[c, dev_me] = dsend[c, t]

        for w in range(WAVES):
            for i in range(heads // 2):
                remote(
                    accs.at[w, c, 2 * i + 1 - core_me],
                    pair.at[w, c, i],
                    a_send.at[w, c],
                    a_recv.at[w, c],
                    (t_me + 1 - 2 * core_me, b_me),
                )

    def pass_on(w, c):
        drain(pair.at[w, c], a_recv.at[w, c])
        per = quads * deep
        for i in range(heads // 2):
            both = accs[w, c, 2 * i + core_me] + pair[w, c, i]
            for g in range(per):
                psend[w, c, i * per + g] = both[g * seqs : (g + 1) * seqs, :].astype(jnp.bfloat16)
        for d in range(deep):
            for chip in range(nt // 2):
                k = w * deep + d
                if k == 0 and chip < DIRECT:
                    continue
                place = chip % (heads // 2) * per + chip // (heads // 2) * deep + d
                mine = jnp.logical_and(lax.div(t_me, 2) == chip, b_me == k)

                @pl.when(jnp.logical_not(mine))
                def _():
                    remote(
                        psend.at[w, c, place],
                        pslot.at[c, chip_me],
                        p_send.at[c],
                        p_recv.at[c],
                        (2 * chip + core_me, k),
                    )

                @pl.when(mine)
                def _():
                    pslot[c, chip_me] = psend[w, c, place]

    for copy in v_copies:
        copy.wait()
    weigh()
    for c in range(chunks + 1):
        if c < chunks:
            multiply(c)
        if c > 0:
            for w in range(WAVES):
                pass_on(w, c - 1)

    def finish(c, ref, count, sem):
        drain(ref.at[pl.ds(0, count - 1)], sem)
        total = jnp.zeros((seqs, piece), jnp.float32)
        for slot in range(count):
            total = total + ref[slot].astype(jnp.float32)
        out_ref[:, pl.ds(c * piece, piece)] = total.astype(jnp.bfloat16)

    for c in range(chunks):
        pl.when(direct)(lambda c=c: finish(c, dslot.at[c], devices, d_recv.at[c]))
        pl.when(jnp.logical_not(direct))(
            lambda c=c: finish(c, pslot.at[c], chips, p_recv.at[c])
        )

    drain_count(central, lambda n: qslot.at[pl.ds(0, n)], heads, q_send)
    drain_count(central, lambda n: kslot.at[pl.ds(0, n)], nt, k_send)
    drain(islot.at[pl.ds(0, devices - 1)], i_send)

    @pl.when(central)
    def _():
        drain(wacc.at[pl.ds(0, (devices - 1) * WAVES * span // 2)], w_send)

    for c in range(chunks):
        drain_count(
            jnp.logical_not(direct),
            lambda n, c=c: pslot.at[c, pl.ds(0, n)],
            chips - DIRECT,
            p_send.at[c],
        )
        drain_count(direct, lambda n, c=c: dsend.at[c, pl.ds(0, n)], 2 * DIRECT, d_send.at[c])
        for w in range(WAVES):
            drain(pair.at[w, c], a_send.at[w, c])


def shards(nt, nb, queries, indices, first_keys, second_keys, values):
    seqs, heads, top = indices.shape
    width_q = queries.shape[2]
    half = width_q // 2
    firsts = first_keys.shape[1]
    sub_count = second_keys.shape[1]
    rows, width = values.shape
    devices = nt * nb
    all_seqs = devices * seqs
    deep = nb // WAVES
    quads = nt // heads
    span = deep * seqs
    assert heads * top == LANES and nt % heads == 0 and heads % 2 == 0
    assert nb % WAVES == 0 and span % 8 == 0
    chunks, pieces = 2, 4
    early = all_seqs <= 256
    held = all_seqs if early else 1
    piece = width // chunks
    per_pair = (heads // 2) * quads * deep
    hbm = pl.BlockSpec(memory_space=pltpu.MemorySpace.HBM)
    dma = pltpu.SemaphoreType.DMA
    return pl.pallas_call(
        functools.partial(kernel, (nt, nb, heads, seqs, top, chunks, pieces, early)),
        out_shape=pltpu.VMEM((seqs, width), jnp.bfloat16),
        in_specs=[hbm] * 5,
        out_specs=pl.BlockSpec(memory_space=pltpu.VMEM),
        scratch_shapes=[
            pltpu.VMEM(queries.shape, queries.dtype),
            pltpu.VMEM(indices.shape, indices.dtype),
            pltpu.VMEM(first_keys.shape, first_keys.dtype),
            pltpu.VMEM((rows, width), jnp.bfloat16),
            pltpu.VMEM((sub_count, half), jnp.bfloat16),
            pltpu.VMEM((devices, firsts, half), jnp.bfloat16),
            pltpu.VMEM((devices, seqs, LANES), jnp.int32),
            pltpu.VMEM((seqs, LANES), jnp.int32),
            pltpu.VMEM((heads, seqs, width_q), jnp.float32),
            pltpu.VMEM((heads, seqs, width_q), jnp.bfloat16),
            pltpu.VMEM((heads * nb, seqs, width_q), jnp.bfloat16),
            pltpu.VMEM((heads * nb * seqs, width_q), jnp.float32),
            pltpu.VMEM((heads * nb * seqs, LANES), jnp.int32),
            pltpu.VMEM((WAVES * span, LANES), jnp.bfloat16),
            pltpu.VMEM((heads * quads, WAVES * span, LANES), jnp.bfloat16),
            pltpu.VMEM((all_seqs, LANES), jnp.int32),
            pltpu.VMEM((all_seqs, LANES), jnp.float32),
            pltpu.VMEM((rows // LANES * (all_seqs + 4), LANES), jnp.float32),
            pltpu.VMEM((all_seqs, rows), jnp.bfloat16),
            pltpu.VMEM((held, rows // LANES, LANES), jnp.bfloat16),
            pltpu.VMEM((held, LANES, LANES), jnp.bfloat16),
            pltpu.VMEM((all_seqs, LANES), jnp.float32),
            pltpu.VMEM((WAVES, chunks, heads, quads * span, piece), jnp.float32),
            pltpu.VMEM((WAVES, chunks, heads // 2, quads * span, piece), jnp.float32),
            pltpu.VMEM((WAVES, chunks, per_pair, seqs, piece), jnp.bfloat16),
            pltpu.VMEM((chunks, devices // 2, seqs, piece), jnp.bfloat16),
            pltpu.VMEM((chunks, 2 * DIRECT, seqs, piece), jnp.bfloat16),
            pltpu.VMEM((chunks, devices, seqs, piece), jnp.bfloat16),
            pltpu.SemaphoreType.REGULAR((nb,)),
            dma((3,)),
            dma((pieces,)),
            dma,
            dma,
            dma,
            dma,
            dma((2,)),
            dma,
            dma,
            dma,
            dma,
            dma((WAVES, chunks)),
            dma((WAVES, chunks)),
            dma((chunks,)),
            dma((chunks,)),
            dma((chunks,)),
            dma((chunks,)),
        ],
        compiler_params=pltpu.CompilerParams(
            collective_id=0, has_side_effects=True, vmem_limit_bytes=56 * 1024 * 1024
        ),
    )(queries, indices, first_keys, second_keys, values)


def solution(mesh):
    placed = (
        P(("table", "batch"), None, None),
        P(("table", "batch"), None, None),
        P(None, ("table", "batch"), None),
        P(),
        P(("table", "batch"), None),
    )
    body = functools.partial(shards, mesh.shape["table"], mesh.shape["batch"])
    return jax.shard_map(
        body, mesh=mesh, in_specs=placed, out_specs=P(("table", "batch"), None), check_vma=False
    )
```
